32 devices in a mesh: groups: 2 (over x), exp: 16 (over z, y, core).
Axes of the slice: x: 2, y: 2, z: 4, core: 2. Of those that a mesh axis runs over, the one named last changes fastest.
Arguments:
- cutouts: float32 [64, 12, 20736], P(('groups', 'exp')), parts along dimension 0, may hold values from -6 to 6
- variance: bfloat16 [64, 12, 20736], P(('groups', 'exp')), parts along dimension 0, may hold values from 0.1 to 30
- offsets: int32 [64, 12, 2], P(('groups', 'exp')), parts along dimension 0, may hold values from 0 to 15
- correlation_tiles: int32 [64, 12], P(('groups', 'exp')), parts along dimension 0, may hold values from 0 to 63, as said below
- slot_valid: int32 [64, 12], P(('groups', 'exp')), parts along dimension 0, may hold values from 0 to 1, as said below
- tile_slot: int32 [128], P('groups'), parts along dimension 0, may hold values from 0 to 63, as said below
Outputs:
- coadd: float32 [128, 128, 128], P(('groups', 'exp')), parts along dimension 0
- depth: float32 [128, 128, 128], P(('groups', 'exp')), parts along dimension 0
The draws below stay inside these ranges and needn't reach their ends.
There are 2 independent parts, one for each index of `groups`. The reference program is written for one: setup_inputs(seed, part) draws one part's arguments, and reference() takes and returns one part's arrays. A program takes and returns all parts, laid end to end along the dimension named above; each array names one. Nothing has to cross between parts.
Inputs may be any that keep to these rules, and one draw needn't show every extreme that they name: `correlation_tiles`: the tile with id t is owned by the device of index tile_slot[t] // 4 along exp. Among the valid slots of one device's 2 exposures at most 3 name tiles of one owner; in every draw one owner is named exactly 3 times by the valid slots of every device. `slot_valid`: each exposure's valid slots come first; at least 6 of its 12 slots are valid. A permutation: tile t is stored in row tile_slot[t] of the outputs.
All inputs are finite; a program needn't handle non-finite values.
Results may differ from the reference program's by a relative error of at most 0.0003.
Values sent between devices are 32-bit elements; how exact they have to be, the bound alone decides.
A program may use at most 128 MiB of HBM per device.

```python
import jax
import jax.numpy as jnp
from jax import lax

P_SIZE = 128
CP = 144
NOFF = 16
SLOTS = 12
EXP_DEV = 2
TILE_DEV = 4
CAP = 3
EXPOSURES = 32
TILES = 64
N_EXP = 16


def layout_tables(key):
    tile_slot = jax.random.permutation(jax.random.fold_in(key, 101), TILES).astype(jnp.int32)
    storage_tile = jnp.argsort(tile_slot).astype(jnp.int32)
    counts = jax.random.randint(jax.random.fold_in(key, 102), (EXPOSURES,), max(1, SLOTS // 2), SLOTS + 1)
    slot_valid = (jnp.arange(SLOTS, dtype=jnp.int32)[None, :] < counts[:, None]).astype(jnp.int32)
    place_count = N_EXP * CAP
    hotness = jax.random.randint(jax.random.fold_in(key, 103), (N_EXP,), 0, 3)
    busiest = jax.random.randint(jax.random.fold_in(key, 104), (), 0, N_EXP)
    hotness = jnp.where(jnp.arange(N_EXP, dtype=jnp.int32) == busiest, 4, hotness)
    places = jnp.arange(place_count, dtype=jnp.int32)
    randoms = jax.random.randint(jax.random.fold_in(key, 105), (N_EXP, place_count), 0, 1024)
    scores = (randoms + hotness[places // CAP][None, :] * 1024) * place_count + places[None, :]
    priority = jnp.argsort(-scores, axis=1).astype(jnp.int32)
    flat_valid = slot_valid.reshape(N_EXP, EXP_DEV * SLOTS)
    slot_rank = jnp.clip(jnp.cumsum(flat_valid, axis=1) - 1, 0, place_count - 1).astype(jnp.int32)
    chosen = jnp.take_along_axis(priority, slot_rank, axis=1)
    owners = chosen // CAP
    within = jax.random.randint(jax.random.fold_in(key, 106), (N_EXP, EXP_DEV * SLOTS), 0, TILE_DEV)
    tile_ids = storage_tile[owners * TILE_DEV + within].reshape(EXPOSURES, SLOTS).astype(jnp.int32)
    return (tile_slot, tile_ids, slot_valid)


def draw_tile_slot(key, part):
    return layout_tables(key)[0]


def draw_correlation_tiles(key, part):
    return layout_tables(key)[1]


def draw_slot_valid(key, part):
    return layout_tables(key)[2]


def draw_variance(key, part):
    rising = 1.0 + 2.0 * jnp.arange(EXPOSURES, dtype=jnp.float32) / max(EXPOSURES - 1, 1)
    levels = rising * jnp.exp(jax.random.uniform(jax.random.fold_in(key, 201), (EXPOSURES,), jnp.float32, -1.15, 1.15))
    pixel_scale = jnp.exp(jax.random.uniform(jax.random.fold_in(key, 202), (EXPOSURES, SLOTS, CP * CP), jnp.float32, -0.35, 0.35))
    return (levels[:, None, None] * pixel_scale).astype(jnp.bfloat16)


def touch_ends(array, key, least, top_value):
    shape = array.shape
    place = [jax.random.randint(jax.random.fold_in(key, axis), (), 0, shape[axis]) for axis in range(len(shape))]
    array = array.at[tuple(place)].set(least)
    longest = shape.index(max(shape))
    place[longest] = (place[longest] + 1) % shape[longest]
    return array.at[tuple(place)].set(top_value)


def level_of(own_key, extent, cuts, least, high):
    factor_of = 1.0
    for dim, parts in cuts:
        heights = jax.random.uniform(jax.random.fold_in(jax.random.fold_in(own_key, 6), dim), (parts,), jnp.float32, least / len(cuts), high / len(cuts))
        factor_of = factor_of * jnp.repeat(jnp.exp(heights), extent[dim] // parts).reshape((-1,) + (1,) * (len(extent) - 1 - dim))
    return factor_of


def normal_values(stream_key, extent, width, limit, split=(), kind=jnp.bfloat16):
    values = width * jax.random.normal(stream_key, extent, jnp.float32)
    if split:
        values = values * level_of(stream_key, extent, split, -0.22, 0.18)
    return jnp.clip(values, -limit, limit).astype(kind)


def setup_inputs(seed: int = 0, part: int = 0) -> dict:
    streams_of = jax.random.split(jax.random.key(seed), 7)
    part_splits = jax.random.split(jax.random.fold_in(streams_of[6], part), 7)
    return {
        "cutouts": normal_values(part_splits[0], (EXPOSURES, SLOTS, CP * CP), 1.0, 6.0, ((0, 16),), jnp.float32),
        "variance": draw_variance(jax.random.fold_in(jax.random.fold_in(streams_of[6], part), 71), part),
        "offsets": touch_ends(jax.random.randint(part_splits[2], (EXPOSURES, SLOTS, 2), 0, NOFF), jax.random.fold_in(part_splits[2], 1), 0, NOFF - 1).astype(jnp.int32),
        "correlation_tiles": draw_correlation_tiles(jax.random.fold_in(jax.random.fold_in(streams_of[6], part), 71), part),
        "slot_valid": draw_slot_valid(jax.random.fold_in(jax.random.fold_in(streams_of[6], part), 71), part),
        "tile_slot": draw_tile_slot(jax.random.fold_in(jax.random.fold_in(streams_of[6], part), 71), part),
    }


clip_ratio = 1.5


def lanczos_table():
    shifts = jnp.arange(NOFF, dtype=jnp.float32) / NOFF
    out_pixel = jnp.arange(P_SIZE, dtype=jnp.float32)
    in_pixel = jnp.arange(CP, dtype=jnp.float32)
    spread = out_pixel[None, :, None] + 8.0 + shifts[:, None, None] - in_pixel[None, None, :]
    return jnp.where(jnp.abs(spread) < 3.0, jnp.sinc(spread) * jnp.sinc(spread / 3.0), 0.0)


def resample(cutout_block, var_block, kernel, square, shift_pairs):
    highest = lax.Precision.HIGHEST
    row_kernel = jnp.take(kernel, shift_pairs[:, 0], axis=0)
    col_kernel = jnp.take(kernel, shift_pairs[:, 1], axis=0)
    row_square = jnp.take(square, shift_pairs[:, 0], axis=0)
    col_square = jnp.take(square, shift_pairs[:, 1], axis=0)
    sampled = jnp.einsum("nij,njk->nik", row_kernel, cutout_block, precision=highest)
    sampled = jnp.einsum("nik,nlk->nil", sampled, col_kernel, precision=highest)
    propagated = jnp.einsum("nij,njk->nik", row_square, var_block.astype(jnp.float32), precision=highest)
    propagated = jnp.einsum("nik,nlk->nil", propagated, col_square, precision=highest)
    inverse = 1.0 / propagated
    return sampled * inverse, inverse


def exposure_weights(variance, slot_valid):
    totals = jnp.sum(variance.astype(jnp.float32), axis=2)
    valid = slot_valid.astype(jnp.float32)
    means = jnp.sum(valid * totals, axis=1) / (jnp.sum(valid, axis=1) * (CP * CP))
    return 1.0 / means


def reference(cutouts, variance, offsets, correlation_tiles, slot_valid, tile_slot):
    kernel = lanczos_table()
    square = kernel * kernel
    weights = exposure_weights(variance, slot_valid)
    average = jnp.sum(weights) / EXPOSURES
    factors = slot_valid.astype(jnp.float32) * (jnp.minimum(weights, clip_ratio * average) / weights)[:, None]
    target_rows = tile_slot[correlation_tiles]
    cut_square = cutouts.reshape(EXPOSURES, SLOTS, CP, CP)
    var_square = variance.reshape(EXPOSURES, SLOTS, CP, CP)

    def absorb(totals, element):
        numerator, denominator = totals
        cutout_block, var_block, shift_pairs, rows_here, factor = element
        scaled, inverse = resample(cutout_block, var_block, kernel, square, shift_pairs)
        numerator = numerator.at[rows_here].add(factor[:, None, None] * scaled)
        denominator = denominator.at[rows_here].add(factor[:, None, None] * inverse)
        return (numerator, denominator), None

    zeros_init = jnp.zeros((TILES, P_SIZE, P_SIZE), jnp.float32)
    (numerator, denominator), _ = lax.scan(absorb, (zeros_init, zeros_init), (cut_square, var_square, offsets, target_rows, factors))
    positive = denominator > 0
    coadd = jnp.where(positive, numerator / jnp.where(positive, denominator, 1.0), 0.0)
    return coadd, denominator
```

```python
import functools

import jax
import jax.numpy as jnp
import numpy as np
from jax import lax
from jax.experimental import pallas as pl
from jax.experimental.pallas import tpu as pltpu
from jax.sharding import PartitionSpec as P

P_SIZE = 128
CP = 144
NOFF = 16
TAPS = 6
FIRST = 6
LANES = 128
ROWS = 8
PAD = 16
PARTS = 2
LAGS = 3
SWAP_EVERY = 4
VMEM_LIMIT = 55_800_000
clip_ratio = 1.5
MESH = pl.DeviceIdType.MESH


def tap_table():
    spread = 8.0 + np.arange(NOFF)[:, None] / NOFF - (FIRST + np.arange(TAPS))[None, :]
    table = np.where(np.abs(spread) < 3.0, np.sinc(spread) * np.sinc(spread / 3.0), 0.0)
    return table.astype(np.float32)


TABLE = tap_table()


def pick_taps(offset):
    taps = []
    for t in range(TAPS):
        value = jnp.zeros(offset.shape, jnp.float32)
        for o in range(NOFF):
            value = jnp.where(offset == o, float(TABLE[o, t]), value)
        taps.append(value)
    return taps


def coadd_kernel(
    dev_count, bits, slot_total, cut_hbm, var_hbm, small_ref,
    coadd_ref, depth_ref, cut_ref, var_ref, weight_src, weight_got, taps_ref,
    cut_mid, var_mid, pick_wide, pick_ref, parts_ref, partial_ref, *rest,
):
    got_refs = rest[:bits]
    load_sem, weight_send, weight_recv, send_sem, recv_sem = rest[bits:]
    slots, exps, _ = cut_hbm.shape
    rows = slots * exps
    tile_dev = slot_total // dev_count
    width = ROWS * P_SIZE
    chunks = P_SIZE // ROWS
    span = ROWS * CP
    ring = partial_ref.shape[0]
    pad = pick_wide.shape[0] // (2 * PARTS)
    me = lax.axis_index("exp")

    barrier = pltpu.get_barrier_semaphore()

    @pl.loop(1, dev_count)
    def _(i):
        pl.semaphore_signal(
            barrier, inc=1, device_id={"exp": lax.rem(me + i, dev_count)}, device_id_type=MESH
        )

    def load(kind, s):
        source, to = ((cut_hbm, cut_ref), (var_hbm, var_ref))[kind]
        return pltpu.make_async_copy(
            source.at[s], to.at[pl.ds(s * exps, exps)], load_sem.at[kind, s]
        )

    for kind in (1, 0):
        for s in range(slots):
            load(kind, s).start()

    of_row = lax.broadcasted_iota(jnp.int32, (rows, slots), 0)
    of_slot = lax.broadcasted_iota(jnp.int32, (rows, slots), 1) == of_row // exps

    def by_row(values):
        column = jnp.zeros((rows, slots), jnp.float32)
        for e in range(exps):
            here = of_slot & (of_row % exps == e)
            column = column + jnp.where(here, values[e].astype(jnp.float32), 0.0)
        return jnp.sum(column, axis=1, keepdims=True)

    def small_row(i):
        return small_ref[i : i + 1, :slots]

    offsets = [by_row([small_row(2 * e + axis) for e in range(exps)]) for axis in range(2)]
    tile = by_row([small_row(2 * exps + e) for e in range(exps)])
    valid = by_row([small_row(3 * exps + e) for e in range(exps)])

    for s in range(slots):
        load(1, s).wait()

    def add_up(g, total):
        var = var_ref[:, pl.ds(pl.multiple_of(g * span, LANES), span)].astype(jnp.float32)
        for k in range(span // LANES):
            total = total + var[:, k * LANES : (k + 1) * LANES]
        return total

    sums = lax.fori_loop(0, CP // ROWS, add_up, jnp.zeros((rows, LANES), jnp.float32))

    exposure = lax.broadcasted_iota(jnp.int32, (rows, 1), 0) % exps
    row_total = jnp.sum(sums, axis=1, keepdims=True) * valid
    own = []
    for e in range(exps):
        total = jnp.sum(jnp.where(exposure == e, row_total, 0.0), axis=0, keepdims=True)
        count = jnp.sum(jnp.where(exposure == e, valid, 0.0), axis=0, keepdims=True)
        own.append(1.0 / (total / (count * (CP * CP))))
    own_sum = functools.reduce(lambda a, b: a + b, own)
    weight_src[...] = jnp.broadcast_to(own_sum, weight_src.shape)
    pl.semaphore_wait(barrier, dev_count - 1)

    def weight_copy(i):
        return pltpu.make_async_remote_copy(
            src_ref=weight_src,
            dst_ref=weight_got.at[i],
            send_sem=weight_send.at[i],
            recv_sem=weight_recv.at[i],
            device_id={"exp": lax.rem(me + i, dev_count)},
            device_id_type=MESH,
        )

    @pl.loop(1, dev_count)
    def _(i):
        weight_copy(i).start()

    for axis in range(2):
        taps = pick_taps(jnp.broadcast_to(offsets[axis], (rows, LANES)))
        for t in range(TAPS):
            taps_ref[axis, 0, t] = taps[t]
            taps_ref[axis, 1, t] = taps[t] * taps[t]

    def columns(g):
        at = pl.ds(pl.multiple_of(g * span, LANES), span)
        for kind in range(2):
            data = (cut_ref, var_ref)[kind][:, at].astype(jnp.float32)
            mid = (cut_mid, var_mid)[kind]
            for r in range(ROWS):
                start = r * CP + FIRST
                got = taps_ref[1, kind, 0] * data[:, start : start + LANES]
                for t in range(1, TAPS):
                    got = got + taps_ref[1, kind, t] * data[:, start + t : start + t + LANES]
                mid[:, pl.ds(pl.multiple_of((g * ROWS + r) * LANES, LANES), LANES)] = got

    row = lax.broadcasted_iota(jnp.int32, (rows, 2 * slot_total), 1)
    place = row // (2 * tile_dev)
    kind_of = (row // tile_dev) % 2
    tile_ids = lax.broadcasted_iota(jnp.int32, (rows, slot_total), 1)
    storage = jnp.sum(
        jnp.where(tile == tile_ids.astype(jnp.float32), small_ref[4 * exps : 4 * exps + 1, :slot_total].astype(jnp.float32), 0.0),
        axis=1,
        keepdims=True,
    )
    pick_wide[...] = jnp.zeros_like(pick_wide)
    parts_ref[...] = jnp.zeros_like(parts_ref)
    for variant in range(2):
        order = list(range(bits))
        if variant == 1 and bits >= 3:
            order[1], order[2] = 2, 1
        owner = jnp.zeros_like(place)
        for b in range(bits):
            owner = owner + ((place // (1 << (bits - 1 - b))) % 2) * (1 << order[b])
        wanted = (owner * tile_dev + row % tile_dev).astype(jnp.float32)
        for kind in range(2):
            hit = jnp.where((kind_of == kind) & (wanted == storage), valid, 0.0)
            for part in range(PARTS):
                base = (kind * PARTS + part) * pad
                pick_wide[base : base + rows, :] = hit
        pick_ref[variant] = pick_wide[...].T.astype(jnp.bfloat16)

    for s in range(slots):
        load(0, s).wait()

    columns(0)
    columns(1)

    @pl.loop(1, dev_count)
    def _(i):
        weight_copy(i).wait()

    weight_got[0] = weight_src[...]
    average = jnp.sum(weight_got[...], axis=0)[0:1, 0:1] / (exps * dev_count)
    factor = jnp.zeros((rows, 1), jnp.float32)
    for e in range(exps):
        factor = jnp.where(exposure == e, jnp.minimum(own[e], clip_ratio * average) / own[e], factor)

    def swapped(c):
        return lax.div(lax.rem(c + SWAP_EVERY - 2, SWAP_EVERY), SWAP_EVERY - 1)

    def stride_of(b, c):
        if bits >= 3 and b == 1:
            return 2 + 2 * swapped(c)
        if bits >= 3 and b == 2:
            return 4 - 2 * swapped(c)
        return 1 << b

    def bit_of(b, c):
        return lax.rem(lax.div(me, stride_of(b, c)), 2)

    def block_copy(b, c):
        n = dev_count >> (b + 1)
        bit = bit_of(b, c)
        if b == 0:
            source = partial_ref.at[lax.rem(c, ring), pl.ds((1 - bit) * n, n)]
        else:
            source = got_refs[b - 1].at[c, pl.ds((1 - bit) * n, n)]
        return pltpu.make_async_remote_copy(
            src_ref=source,
            dst_ref=got_refs[b].at[c],
            send_sem=send_sem.at[b, c],
            recv_sem=recv_sem.at[b, c],
            device_id={"exp": me + (1 - 2 * bit) * stride_of(b, c)},
            device_id_type=MESH,
        )

    def kept(b, c):
        n = dev_count >> (b + 1)
        if b == 0:
            return partial_ref[lax.rem(c, ring), pl.ds(bit_of(b, c) * n, n)]
        return got_refs[b - 1][c, pl.ds(bit_of(b, c) * n, n)]

    @pl.loop(0, chunks + LAGS * bits - LAGS + 1)
    def _(step):
        @pl.when(step < chunks)
        def _():
            c = step
            columns(c + 2)
            for r in range(ROWS):
                value = []
                for kind in range(2):
                    mid = (cut_mid, var_mid)[kind]
                    got = None
                    for t in range(TAPS):
                        from_row = c * ROWS + r + FIRST + t
                        at = pl.ds(pl.multiple_of(from_row * LANES, LANES), LANES)
                        term = taps_ref[0, kind, t] * mid[:, at]
                        got = term if t == 0 else got + term
                    value.append(got)
                inverse = 1.0 / value[1]
                scaled = value[0] * inverse
                for kind in range(2):
                    piece_of = (scaled, inverse)[kind] * factor
                    for part in range(PARTS):
                        base = (kind * PARTS + part) * pad
                        piece = piece_of.astype(jnp.bfloat16)
                        parts_ref[base : base + rows, r * LANES : (r + 1) * LANES] = piece
                        piece_of = piece_of - piece.astype(jnp.float32)

            @pl.when(c >= ring)
            def _():
                block_copy(0, c - ring).wait_send()

            added = jnp.dot(
                pick_ref[swapped(c)], parts_ref[...], preferred_element_type=jnp.float32
            )
            partial_ref[lax.rem(c, ring)] = added.reshape(dev_count, 2 * tile_dev, width)
            block_copy(0, c).start()

        for b in range(1, bits + 1):
            c = step - (LAGS * (b - 1) + 1)

            @pl.when((c >= 0) & (c < chunks))
            def _(b=b, c=c):
                block_copy(b - 1, c).wait_recv()
                total = got_refs[b - 1][c] + kept(b - 1, c)
                if b < bits:
                    got_refs[b - 1][c] = total
                    block_copy(b, c).start()
                else:
                    at = pl.ds(pl.multiple_of(c * width, LANES), width)
                    numerator = total[0, :tile_dev]
                    denominator = total[0, tile_dev:]
                    positive = denominator > 0
                    coadd_ref[:, at] = jnp.where(
                        positive, numerator / jnp.where(positive, denominator, 1.0), 0.0
                    )
                    depth_ref[:, at] = denominator

    @pl.loop(chunks - ring, chunks)
    def _(c):
        block_copy(0, c).wait_send()

    @pl.loop(0, chunks)
    def _(c):
        for b in range(1, bits):
            block_copy(b, c).wait_send()


def shards(cutouts, variance, offsets, correlation_tiles, slot_valid, tile_slot):
    dev_count = lax.axis_size("exp")
    exps, slots, pixels = cutouts.shape
    rows = exps * slots
    tile_total = tile_slot.shape[0]
    tile_dev = tile_total // dev_count
    bits = dev_count.bit_length() - 1
    chunks = P_SIZE // ROWS
    width = ROWS * P_SIZE
    ring = min(chunks, 4)
    depth = 2 * PARTS * (-(-rows // PAD) * PAD)
    area = P_SIZE * P_SIZE

    lanes = max(LANES, tile_total)
    small = jnp.concatenate(
        [
            jnp.pad(a, ((0, 0), (0, lanes - a.shape[1])))
            for a in (
                jnp.swapaxes(offsets, 1, 2).reshape(2 * exps, slots),
                correlation_tiles,
                slot_valid,
                tile_slot.reshape(1, tile_total),
            )
        ],
        axis=0,
    )
    whole = pl.BlockSpec(memory_space=pltpu.VMEM)
    far = pl.BlockSpec(memory_space=pltpu.HBM)
    coadd, depth_sum = pl.pallas_call(
        functools.partial(coadd_kernel, dev_count, bits, tile_total),
        out_shape=(jax.ShapeDtypeStruct((tile_dev, area), jnp.float32),) * 2,
        in_specs=[far] * 2 + [whole],
        out_specs=(whole,) * 2,
        scratch_shapes=[
            pltpu.VMEM((rows, pixels), cutouts.dtype),
            pltpu.VMEM((rows, pixels), variance.dtype),
            pltpu.VMEM((ROWS, LANES), jnp.float32),
            pltpu.VMEM((dev_count, ROWS, LANES), jnp.float32),
            pltpu.VMEM((2, 2, TAPS, rows, LANES), jnp.float32),
            pltpu.VMEM((rows, CP * P_SIZE), jnp.float32),
            pltpu.VMEM((rows, CP * P_SIZE), jnp.float32),
            pltpu.VMEM((depth, 2 * tile_total), jnp.float32),
            pltpu.VMEM((2, 2 * tile_total, depth), jnp.bfloat16),
            pltpu.VMEM((depth, width), jnp.bfloat16),
            pltpu.VMEM((ring, dev_count, 2 * tile_dev, width), jnp.float32),
        ]
        + [
            pltpu.VMEM((chunks, dev_count >> (b + 1), 2 * tile_dev, width), jnp.float32)
            for b in range(bits)
        ]
        + [
            pltpu.SemaphoreType.DMA((2, slots)),
            pltpu.SemaphoreType.DMA((dev_count,)),
            pltpu.SemaphoreType.DMA((dev_count,)),
            pltpu.SemaphoreType.DMA((bits, chunks)),
            pltpu.SemaphoreType.DMA((bits, chunks)),
        ],
        compiler_params=pltpu.CompilerParams(
            collective_id=0, has_side_effects=True, vmem_limit_bytes=VMEM_LIMIT
        ),
        name="coadd",
    )(
        jnp.swapaxes(cutouts, 0, 1),
        jnp.swapaxes(variance, 0, 1),
        small,
    )
    shape = (tile_dev, P_SIZE, P_SIZE)
    return (coadd.reshape(shape), depth_sum.reshape(shape))


def solution(mesh):
    in_specs = (
        P(("groups", "exp"), None, None),
        P(("groups", "exp"), None, None),
        P(("groups", "exp"), None, None),
        P(("groups", "exp"), None),
        P(("groups", "exp"), None),
        P("groups"),
    )
    out_specs = (P(("groups", "exp"), None, None), P(("groups", "exp"), None, None))
    return jax.shard_map(shards, mesh=mesh, in_specs=in_specs, out_specs=out_specs, check_vma=False)
```

```python
import functools

import jax
import jax.numpy as jnp
import numpy as np
from jax import lax
from jax.experimental import pallas as pl
from jax.experimental.pallas import tpu as pltpu
from jax.sharding import PartitionSpec as P

P_SIZE = 128
CP = 144
NOFF = 16
TAPS = 6
FIRST = 6
LANES = 128
ROWS = 8
PAD = 16
PARTS = 2
ALL_RING = 16
AHEAD = 4
LATE = (1,)
LAGS = (1, 4, 8, 20)
LATE_LAGS = (1, 3, 7, 16)
LAST_PER_STEP = 3
VMEM_LIMIT = 55_800_000
clip_ratio = 1.5
MESH = pl.DeviceIdType.MESH


def tap_table():
    spread = 8.0 + np.arange(NOFF)[:, None] / NOFF - (FIRST + np.arange(TAPS))[None, :]
    table = np.where(np.abs(spread) < 3.0, np.sinc(spread) * np.sinc(spread / 3.0), 0.0)
    return table.astype(np.float32)


TABLE = tap_table()


def pick_taps(offset):
    taps = []
    for t in range(TAPS):
        value = jnp.zeros(offset.shape, jnp.float32)
        for o in range(NOFF):
            value = jnp.where(offset == o, float(TABLE[o, t]), value)
        taps.append(value)
    return taps


def stage_lags(lags, bits):
    middle = [lags[2] + 4 * i for i in range(bits - 3)]
    return list(lags[:2]) + middle + [middle[-1] + lags[3] - lags[2]]


def coadd_kernel(
    dev_count, bits, slot_total, cut_hbm, var_hbm, small_ref,
    coadd_ref, depth_ref, cut_ref, var_ref, weight_src, weight_got, taps_ref,
    cut_mid, var_mid, value_ref, pick_wide, pick_ref, parts_ref, partial_ref, *rest,
):
    got_refs = rest[:bits]
    load_sem, weight_send, weight_recv, send_sem, recv_sem, last_send, last_recv = rest[bits:]
    slots, exps, _ = cut_hbm.shape
    rows = slots * exps
    tile_dev = slot_total // dev_count
    width = ROWS * P_SIZE
    chunks = P_SIZE // ROWS
    span = ROWS * CP
    ring = partial_ref.shape[0]
    pad = pick_wide.shape[0] // (2 * PARTS)
    me = lax.axis_index("exp")

    def bit_order(late):
        return [0, *range(2, bits), 1] if late else list(range(bits))

    barrier = pltpu.get_barrier_semaphore()

    @pl.loop(1, dev_count)
    def _(i):
        pl.semaphore_signal(
            barrier, inc=1, device_id={"exp": lax.rem(me + i, dev_count)}, device_id_type=MESH
        )

    def load(kind, s):
        source, to = ((cut_hbm, cut_ref), (var_hbm, var_ref))[kind]
        return pltpu.make_async_copy(
            source.at[s], to.at[pl.ds(s * exps, exps)], load_sem.at[kind, s]
        )

    for kind in (1, 0):
        for s in range(slots):
            load(kind, s).start()

    of_row = lax.broadcasted_iota(jnp.int32, (rows, slots), 0)
    of_slot = lax.broadcasted_iota(jnp.int32, (rows, slots), 1) == of_row // exps

    def by_row(values):
        column = jnp.zeros((rows, slots), jnp.float32)
        for e in range(exps):
            here = of_slot & (of_row % exps == e)
            column = column + jnp.where(here, values[e].astype(jnp.float32), 0.0)
        return jnp.sum(column, axis=1, keepdims=True)

    def small_row(i):
        return small_ref[i : i + 1, :slots]

    offsets = [by_row([small_row(2 * e + axis) for e in range(exps)]) for axis in range(2)]
    tile = by_row([small_row(2 * exps + e) for e in range(exps)])
    valid = by_row([small_row(3 * exps + e) for e in range(exps)])

    for s in range(slots):
        load(1, s).wait()

    def add_up(g, total):
        var = var_ref[:, pl.ds(pl.multiple_of(g * span, LANES), span)].astype(jnp.float32)
        for k in range(span // LANES):
            total = total + var[:, k * LANES : (k + 1) * LANES]
        return total

    sums = lax.fori_loop(0, CP // ROWS, add_up, jnp.zeros((rows, LANES), jnp.float32))

    exposure = lax.broadcasted_iota(jnp.int32, (rows, 1), 0) % exps
    row_total = jnp.sum(sums, axis=1, keepdims=True) * valid
    own = []
    for e in range(exps):
        total = jnp.sum(jnp.where(exposure == e, row_total, 0.0), axis=0, keepdims=True)
        count = jnp.sum(jnp.where(exposure == e, valid, 0.0), axis=0, keepdims=True)
        own.append(1.0 / (total / (count * (CP * CP))))
    own_sum = functools.reduce(lambda a, b: a + b, own)
    weight_src[...] = jnp.broadcast_to(own_sum, weight_src.shape)
    pl.semaphore_wait(barrier, dev_count - 1)

    def weight_copy(i):
        return pltpu.make_async_remote_copy(
            src_ref=weight_src,
            dst_ref=weight_got.at[i],
            send_sem=weight_send.at[i],
            recv_sem=weight_recv.at[i],
            device_id={"exp": lax.rem(me + i, dev_count)},
            device_id_type=MESH,
        )

    @pl.loop(1, dev_count)
    def _(i):
        weight_copy(i).start()

    for axis in range(2):
        taps = pick_taps(jnp.broadcast_to(offsets[axis], (rows, LANES)))
        for t in range(TAPS):
            taps_ref[axis, 0, t] = taps[t]
            taps_ref[axis, 1, t] = taps[t] * taps[t]

    def columns(g):
        at = pl.ds(pl.multiple_of(g * span, LANES), span)
        for kind in range(2):
            data = (cut_ref, var_ref)[kind][:, at].astype(jnp.float32)
            mid = (cut_mid, var_mid)[kind]
            for r in range(ROWS):
                start = r * CP + FIRST
                got = taps_ref[1, kind, 0] * data[:, start : start + LANES]
                for t in range(1, TAPS):
                    got = got + taps_ref[1, kind, t] * data[:, start + t : start + t + LANES]
                mid[:, pl.ds(pl.multiple_of((g * ROWS + r) * LANES, LANES), LANES)] = got

    row = lax.broadcasted_iota(jnp.int32, (rows, 2 * slot_total), 1)
    place = row // (2 * tile_dev)
    kind_of = (row // tile_dev) % 2
    tile_ids = lax.broadcasted_iota(jnp.int32, (rows, slot_total), 1)
    storage = jnp.sum(
        jnp.where(tile == tile_ids.astype(jnp.float32), small_ref[4 * exps : 4 * exps + 1, :slot_total].astype(jnp.float32), 0.0),
        axis=1,
        keepdims=True,
    )
    pick_wide[...] = jnp.zeros_like(pick_wide)
    parts_ref[...] = jnp.zeros_like(parts_ref)
    for late in range(2):
        order = bit_order(late)
        owner = jnp.zeros_like(place)
        for b in range(bits):
            apart = (place // (1 << (bits - 1 - b))) % 2
            mine = lax.rem(lax.div(me, 1 << order[b]), 2)
            owner = owner + ((apart + mine) % 2) * (1 << order[b])
        wanted = (owner * tile_dev + row % tile_dev).astype(jnp.float32)
        for kind in range(2):
            hit = jnp.where((kind_of == kind) & (wanted == storage), valid, 0.0)
            for part in range(PARTS):
                base = (kind * PARTS + part) * pad
                pick_wide[base : base + rows, :] = hit
        pick_ref[late] = pick_wide[...].T.astype(jnp.bfloat16)

    for s in range(slots):
        load(0, s).wait()

    def resample(c):
        for r in range(ROWS):
            value = []
            for kind in range(2):
                mid = (cut_mid, var_mid)[kind]
                got = None
                for t in range(TAPS):
                    from_row = c * ROWS + r + FIRST + t
                    at = pl.ds(pl.multiple_of(from_row * LANES, LANES), LANES)
                    term = taps_ref[0, kind, t] * mid[:, at]
                    got = term if t == 0 else got + term
                value.append(got)
            inverse = 1.0 / value[1]
            at = pl.ds(pl.multiple_of(c * width + r * LANES, LANES), LANES)
            value_ref[0, :, at] = value[0] * inverse
            value_ref[1, :, at] = inverse

    columns(0)
    columns(1)

    @pl.loop(0, AHEAD)
    def _(c):
        columns(c + 2)
        resample(c)

    @pl.loop(1, dev_count)
    def _(i):
        weight_copy(i).wait()

    weight_got[0] = weight_src[...]
    average = jnp.sum(weight_got[...], axis=0)[0:1, 0:1] / (exps * dev_count)
    factor = jnp.zeros((rows, 1), jnp.float32)
    for e in range(exps):
        factor = jnp.where(exposure == e, jnp.minimum(own[e], clip_ratio * average) / own[e], factor)

    def partner(stride):
        return {"exp": me + (1 - 2 * lax.rem(lax.div(me, stride), 2)) * stride}

    def stage_copy(b, c, late):
        keep = dev_count >> (b + 1)
        skip = 1 if b == 1 and not late else 0
        source = partial_ref.at[lax.rem(c, ring)] if b == 0 else got_refs[b - 1].at[c]
        return pltpu.make_async_remote_copy(
            src_ref=source.at[pl.ds(keep + skip, keep - skip)],
            dst_ref=got_refs[b].at[c, pl.ds(skip, keep - skip)],
            send_sem=send_sem.at[b, c],
            recv_sem=recv_sem.at[b, c],
            device_id=partner(1 << bit_order(late)[b]),
            device_id_type=MESH,
        )

    def last_copy(c):
        keep = dev_count >> 2
        return pltpu.make_async_remote_copy(
            src_ref=got_refs[0].at[c, pl.ds(keep, 1)],
            dst_ref=got_refs[1].at[c, pl.ds(0, 1)],
            send_sem=last_send.at[c],
            recv_sem=last_recv.at[c],
            device_id=partner(2),
            device_id_type=MESH,
        )

    def is_late(c):
        return functools.reduce(lambda a, b: a | b, [c == late for late in LATE])

    def merge(b, c, late):
        keep = dev_count >> (b + 1)
        stage_copy(b, c, late).wait_recv()
        if b == 0:
            got_refs[0][c] = got_refs[0][c] + partial_ref[lax.rem(c, ring), pl.ds(0, keep)]
        elif b == 1 and not late:
            at = pl.ds(1, keep - 1)
            got_refs[1][c, at] = got_refs[1][c, at] + got_refs[0][c, at]
        elif b == 2 and not late:
            got_refs[2][c, pl.ds(0, 1)] = got_refs[2][c, pl.ds(0, 1)] + got_refs[0][c, pl.ds(0, 1)]
            if keep > 1:
                at = pl.ds(1, keep - 1)
                got_refs[2][c, at] = got_refs[2][c, at] + got_refs[1][c, at]
        elif b < bits - 1:
            got_refs[b][c] = got_refs[b][c] + got_refs[b - 1][c, pl.ds(0, keep)]
        if b < bits - 1:
            stage_copy(b + 1, c, late).start()
            return
        total = got_refs[b][c, 0] + got_refs[b - 1][c, 0]
        if not late:
            last_copy(c).wait_recv()
            total = total + got_refs[1][c, 0]
        at = pl.ds(pl.multiple_of(c * width, LANES), width)
        numerator = total[:tile_dev]
        denominator = total[tile_dev:]
        positive = denominator > 0
        coadd_ref[:, at] = jnp.where(
            positive, numerator / jnp.where(positive, denominator, 1.0), 0.0
        )
        depth_ref[:, at] = denominator

    def produce(c):
        for r in range(ROWS):
            for kind in range(2):
                at = pl.ds(pl.multiple_of(c * width + r * LANES, LANES), LANES)
                piece_of = value_ref[kind, :, at] * factor
                for part in range(PARTS):
                    base = (kind * PARTS + part) * pad
                    piece = piece_of.astype(jnp.bfloat16)
                    parts_ref[base : base + rows, r * LANES : (r + 1) * LANES] = piece
                    piece_of = piece_of - piece.astype(jnp.float32)

        if ring < chunks:

            @pl.when(c >= ring)
            def _():
                stage_copy(0, c - ring, False).wait_send()

        added = jnp.dot(
            pick_ref[is_late(c).astype(jnp.int32)],
            parts_ref[...],
            preferred_element_type=jnp.float32,
        )
        partial_ref[lax.rem(c, ring)] = added.reshape(dev_count, 2 * tile_dev, width)
        stage_copy(0, c, False).start()

    lags, late_lags = stage_lags(LAGS, bits), stage_lags(LATE_LAGS, bits)

    @pl.loop(0, chunks + max(lags[-1], late_lags[-1]))
    def _(step):
        @pl.when((step >= AHEAD) & (step < chunks))
        def _():
            columns(step + 2)
            resample(step)

        @pl.when(step < chunks)
        def _():
            produce(step)

        for b in range(bits):
            for late in (False, True):
                c = step - (late_lags if late else lags)[b]
                kind_here = is_late(c) if late else jnp.logical_not(is_late(c))

                @pl.when((c >= 0) & (c < chunks) & kind_here)
                def _(b=b, c=c, late=late):
                    merge(b, c, late)

        for i in range(LAST_PER_STEP):
            c = (step - chunks) * LAST_PER_STEP + i

            @pl.when((c >= 0) & (c < chunks) & jnp.logical_not(is_late(c)))
            def _(c=c):
                last_copy(c).start()

    @pl.loop(chunks - ring, chunks)
    def _(c):
        stage_copy(0, c, False).wait_send()

    @pl.loop(0, chunks)
    def _(c):
        for late in (False, True):

            @pl.when(is_late(c) if late else jnp.logical_not(is_late(c)))
            def _(late=late):
                for b in range(1, bits):
                    stage_copy(b, c, late).wait_send()
                if not late:
                    last_copy(c).wait_send()


def shards(cutouts, variance, offsets, correlation_tiles, slot_valid, tile_slot):
    dev_count = lax.axis_size("exp")
    exps, slots, pixels = cutouts.shape
    rows = exps * slots
    tile_total = tile_slot.shape[0]
    tile_dev = tile_total // dev_count
    bits = dev_count.bit_length() - 1
    chunks = P_SIZE // ROWS
    width = ROWS * P_SIZE
    ring = chunks if dev_count <= ALL_RING else min(chunks, 4)
    depth = 2 * PARTS * (-(-rows // PAD) * PAD)
    area = P_SIZE * P_SIZE

    lanes = max(LANES, tile_total)
    small = jnp.concatenate(
        [
            jnp.pad(a, ((0, 0), (0, lanes - a.shape[1])))
            for a in (
                jnp.swapaxes(offsets, 1, 2).reshape(2 * exps, slots),
                correlation_tiles,
                slot_valid,
                tile_slot.reshape(1, tile_total),
            )
        ],
        axis=0,
    )
    whole = pl.BlockSpec(memory_space=pltpu.VMEM)
    far = pl.BlockSpec(memory_space=pltpu.HBM)
    coadd, depth_sum = pl.pallas_call(
        functools.partial(coadd_kernel, dev_count, bits, tile_total),
        out_shape=(jax.ShapeDtypeStruct((tile_dev, area), jnp.float32),) * 2,
        in_specs=[far] * 2 + [whole],
        out_specs=(whole,) * 2,
        scratch_shapes=[
            pltpu.VMEM((rows, pixels), cutouts.dtype),
            pltpu.VMEM((rows, pixels), variance.dtype),
            pltpu.VMEM((ROWS, LANES), jnp.float32),
            pltpu.VMEM((dev_count, ROWS, LANES), jnp.float32),
            pltpu.VMEM((2, 2, TAPS, rows, LANES), jnp.float32),
            pltpu.VMEM((rows, CP * P_SIZE), jnp.float32),
            pltpu.VMEM((rows, CP * P_SIZE), jnp.float32),
            pltpu.VMEM((2, rows, area), jnp.float32),
            pltpu.VMEM((depth, 2 * tile_total), jnp.float32),
            pltpu.VMEM((2, 2 * tile_total, depth), jnp.bfloat16),
            pltpu.VMEM((depth, width), jnp.bfloat16),
            pltpu.VMEM((ring, dev_count, 2 * tile_dev, width), jnp.float32),
        ]
        + [
            pltpu.VMEM((chunks, dev_count >> (b + 1), 2 * tile_dev, width), jnp.float32)
            for b in range(bits)
        ]
        + [
            pltpu.SemaphoreType.DMA((2, slots)),
            pltpu.SemaphoreType.DMA((dev_count,)),
            pltpu.SemaphoreType.DMA((dev_count,)),
            pltpu.SemaphoreType.DMA((bits, chunks)),
            pltpu.SemaphoreType.DMA((bits, chunks)),
            pltpu.SemaphoreType.DMA((chunks,)),
            pltpu.SemaphoreType.DMA((chunks,)),
        ],
        compiler_params=pltpu.CompilerParams(
            collective_id=0, has_side_effects=True, vmem_limit_bytes=VMEM_LIMIT
        ),
        name="coadd",
    )(
        jnp.swapaxes(cutouts, 0, 1),
        jnp.swapaxes(variance, 0, 1),
        small,
    )
    shape = (tile_dev, P_SIZE, P_SIZE)
    return (coadd.reshape(shape), depth_sum.reshape(shape))


def solution(mesh):
    in_specs = (
        P(("groups", "exp"), None, None),
        P(("groups", "exp"), None, None),
        P(("groups", "exp"), None, None),
        P(("groups", "exp"), None),
        P(("groups", "exp"), None),
        P("groups"),
    )
    out_specs = (P(("groups", "exp"), None, None), P(("groups", "exp"), None, None))
    return jax.shard_map(shards, mesh=mesh, in_specs=in_specs, out_specs=out_specs, check_vma=False)
```

```python
import functools

import jax
import jax.numpy as jnp
import numpy as np
from jax import lax
from jax.experimental import pallas as pl
from jax.experimental.pallas import tpu as pltpu
from jax.sharding import PartitionSpec as P

P_SIZE = 128
CP = 144
NOFF = 16
TAPS = 6
FIRST = 6
LANES = 128
ROWS = 8
PAD = 16
PARTS = 2
ALL_RING = 16
AHEAD = 3
EARLY = 1
LATE = (0, 2)
LAGS = (1, 4, 7, 18)
LATE_LAGS = (1, 6, 8, 19)
LAST_FROM = 1
LAST_PER_STEP = 4
VMEM_LIMIT = 55_800_000
VMEM_MOST = 60 * 1024 * 1024
clip_ratio = 1.5
MESH = pl.DeviceIdType.MESH


def tap_table():
    spread = 8.0 + np.arange(NOFF)[:, None] / NOFF - (FIRST + np.arange(TAPS))[None, :]
    table = np.where(np.abs(spread) < 3.0, np.sinc(spread) * np.sinc(spread / 3.0), 0.0)
    return table.astype(np.float32)


TABLE = tap_table()


def pick_taps(offset):
    taps = []
    for t in range(TAPS):
        value = jnp.zeros(offset.shape, jnp.float32)
        for o in range(NOFF):
            value = jnp.where(offset == o, float(TABLE[o, t]), value)
        taps.append(value)
    return taps


def unused(body):
    return body


def stage_lags(lags, bits):
    middle = [lags[2] + 4 * i for i in range(bits - 3)]
    return list(lags[:2]) + middle + [middle[-1] + lags[3] - lags[2]]


def coadd_kernel(
    dev_count, bits, slot_total, early, cut_hbm, var_hbm, small_ref,
    coadd_ref, depth_ref, cut_ref, var_ref, weight_src, weight_got, taps_ref,
    cut_mid, var_mid, value_ref, early_ref, early_got, pick_wide, pick_ref, parts_ref, partial_ref, *rest,
):
    got_refs = rest[:bits]
    load_sem, weight_send, weight_recv, send_sem, recv_sem, last_send, last_recv = rest[bits:]
    slots, exps, _ = cut_hbm.shape
    rows = slots * exps
    tile_dev = slot_total // dev_count
    width = ROWS * P_SIZE
    chunks = P_SIZE // ROWS
    span = ROWS * CP
    ring = partial_ref.shape[0]
    pad = pick_wide.shape[0] // PARTS
    me = lax.axis_index("exp")

    def bit_order(late):
        return [0, *range(2, bits), 1] if late else list(range(bits))

    barrier = pltpu.get_barrier_semaphore()

    @pl.loop(1, dev_count)
    def _(i):
        pl.semaphore_signal(
            barrier, inc=1, device_id={"exp": lax.rem(me + i, dev_count)}, device_id_type=MESH
        )

    def load(kind, s):
        source, to = ((cut_hbm, cut_ref), (var_hbm, var_ref))[kind]
        return pltpu.make_async_copy(
            source.at[s], to.at[pl.ds(s * exps, exps)], load_sem.at[kind, s]
        )

    for kind in (1, 0):
        for s in range(slots):
            load(kind, s).start()

    of_row = lax.broadcasted_iota(jnp.int32, (rows, slots), 0)
    of_slot = lax.broadcasted_iota(jnp.int32, (rows, slots), 1) == of_row // exps

    def by_row(values):
        column = jnp.zeros((rows, slots), jnp.float32)
        for e in range(exps):
            here = of_slot & (of_row % exps == e)
            column = column + jnp.where(here, values[e].astype(jnp.float32), 0.0)
        return jnp.sum(column, axis=1, keepdims=True)

    def small_row(i):
        return small_ref[i : i + 1, :slots]

    offsets = [by_row([small_row(2 * e + axis) for e in range(exps)]) for axis in range(2)]
    tile = by_row([small_row(2 * exps + e) for e in range(exps)])
    valid = by_row([small_row(3 * exps + e) for e in range(exps)])

    for s in range(slots):
        load(1, s).wait()

    def add_up(g, total):
        var = var_ref[:, pl.ds(pl.multiple_of(g * span, LANES), span)].astype(jnp.float32)
        for k in range(span // LANES):
            total = total + var[:, k * LANES : (k + 1) * LANES]
        return total

    sums = lax.fori_loop(0, CP // ROWS, add_up, jnp.zeros((rows, LANES), jnp.float32))

    exposure = lax.broadcasted_iota(jnp.int32, (rows, 1), 0) % exps
    row_total = jnp.sum(sums, axis=1, keepdims=True) * valid
    own = []
    for e in range(exps):
        total = jnp.sum(jnp.where(exposure == e, row_total, 0.0), axis=0, keepdims=True)
        count = jnp.sum(jnp.where(exposure == e, valid, 0.0), axis=0, keepdims=True)
        own.append(1.0 / (total / (count * (CP * CP))))
    weight_row = lax.broadcasted_iota(jnp.int32, weight_src.shape, 0)
    weight_src[...] = functools.reduce(
        lambda a, b: a + b, [jnp.where(weight_row == e, own[e], 0.0) for e in range(exps)]
    )
    pl.semaphore_wait(barrier, dev_count - 1)

    def weight_copy(i):
        return pltpu.make_async_remote_copy(
            src_ref=weight_src,
            dst_ref=weight_got.at[i],
            send_sem=weight_send.at[i],
            recv_sem=weight_recv.at[i],
            device_id={"exp": lax.rem(me + i, dev_count)},
            device_id_type=MESH,
        )

    @pl.loop(1, dev_count)
    def _(i):
        weight_copy(i).start()

    for axis in range(2):
        taps = pick_taps(jnp.broadcast_to(offsets[axis], (rows, LANES)))
        for t in range(TAPS):
            taps_ref[axis, 0, t] = taps[t]
            taps_ref[axis, 1, t] = taps[t] * taps[t]

    lane = lax.broadcasted_iota(jnp.int32, (rows, LANES), 1)

    def shifted(blocks, by):
        turned = [pltpu.roll(block, LANES - by, axis=1) for block in blocks]
        return [
            jnp.where(lane < LANES - by, here, beyond)
            for here, beyond in zip(turned, turned[1:] + turned[-1:])
        ]

    def columns(g):
        at = pl.ds(pl.multiple_of(g * span, LANES), span)
        for kind in range(2):
            data = (cut_ref, var_ref)[kind][:, at].astype(jnp.float32)
            mid = (cut_mid, var_mid)[kind]
            first = [data[:, k * LANES : (k + 1) * LANES] for k in range(span // LANES)]
            second, third = shifted(first, 1), shifted(first, 2)
            tap = [taps_ref[1, kind, t] for t in range(TAPS)]
            low, high = (
                [tap[t] * x + tap[t + 1] * y + tap[t + 2] * z for x, y, z in zip(first, second, third)]
                for t in (0, 3)
            )
            for r in range(ROWS):
                got = None
                for part, start in ((low, FIRST), (high, FIRST + 3)):
                    block, by = divmod(r * CP + start, LANES)
                    near = pltpu.roll(part[block], LANES - by, axis=1)
                    far = pltpu.roll(part[block + 1], LANES - by, axis=1)
                    term = jnp.where(lane < LANES - by, near, far)
                    got = term if got is None else got + term
                mid[:, pl.ds(pl.multiple_of((g * ROWS + r) * LANES, LANES), LANES)] = got

    row = lax.broadcasted_iota(jnp.int32, (rows, 2 * slot_total), 1)
    place = row // (2 * tile_dev)
    kind_of = (row // tile_dev) % 2
    tile_ids = lax.broadcasted_iota(jnp.int32, (rows, slot_total), 1)
    storage = jnp.sum(
        jnp.where(tile == tile_ids.astype(jnp.float32), small_ref[4 * exps : 4 * exps + 1, :slot_total].astype(jnp.float32), 0.0),
        axis=1,
        keepdims=True,
    )
    pick_wide[...] = jnp.zeros_like(pick_wide)
    parts_ref[...] = jnp.zeros_like(parts_ref)
    for late in range(2):
        order = bit_order(late)
        owner = jnp.zeros_like(place)
        for b in range(bits):
            apart = (place // (1 << (bits - 1 - b))) % 2
            mine = lax.rem(lax.div(me, 1 << order[b]), 2)
            owner = owner + ((apart + mine) % 2) * (1 << order[b])
        wanted = (owner * tile_dev + row % tile_dev).astype(jnp.float32)
        for kind in range(2):
            hit = jnp.where((kind_of == kind) & (wanted == storage), valid, 0.0)
            for part in range(PARTS):
                base = part * pad + kind * rows
                pick_wide[base : base + rows, :] = hit
        pick_ref[late] = pick_wide[...].T.astype(jnp.bfloat16)

    for s in range(slots):
        load(0, s).wait()

    def resample(c):
        for r in range(ROWS):
            value = []
            for kind in range(2):
                mid = (cut_mid, var_mid)[kind]
                got = None
                for t in range(TAPS):
                    from_row = c * ROWS + r + FIRST + t
                    at = pl.ds(pl.multiple_of(from_row * LANES, LANES), LANES)
                    term = taps_ref[0, kind, t] * mid[:, at]
                    got = term if t == 0 else got + term
                value.append(got)
            inverse = 1.0 / value[1]
            at = pl.ds(pl.multiple_of(c * width + r * LANES, LANES), LANES)
            value_ref[:rows, at] = value[0] * inverse
            value_ref[rows:, at] = inverse

    columns(0)
    columns(1)

    @pl.loop(0, early)
    def _(c):
        columns(c + 2)
        resample(c)

    def partner(stride):
        return {"exp": me + (1 - 2 * lax.rem(lax.div(me, stride), 2)) * stride}

    def is_late(c):
        return functools.reduce(lambda a, b: a | b, [c == late for late in LATE])

    def partial_of(c, scale):
        both = jnp.concatenate([scale, scale], axis=0)
        for r in range(ROWS):
            at = pl.ds(pl.multiple_of(c * width + r * LANES, LANES), LANES)
            piece_of = value_ref[:, at] * both
            for part in range(PARTS):
                piece = piece_of.astype(jnp.bfloat16)
                parts_ref[part * pad : part * pad + 2 * rows, r * LANES : (r + 1) * LANES] = piece
                piece_of = piece_of - piece.astype(jnp.float32)
        added = jnp.dot(
            pick_ref[is_late(c).astype(jnp.int32)],
            parts_ref[...],
            preferred_element_type=jnp.float32,
        )
        return added.reshape(dev_count, 2 * tile_dev, width)

    def early_copy(c):
        half = dev_count // 2
        return pltpu.make_async_remote_copy(
            src_ref=early_ref.at[c, :, pl.ds(half, half)],
            dst_ref=early_got.at[c],
            send_sem=send_sem.at[0, c],
            recv_sem=recv_sem.at[0, c],
            device_id=partner(1),
            device_id_type=MESH,
        )

    @pl.loop(0, early) if early else unused
    def _(c):
        for e in range(exps):
            early_ref[c, e] = partial_of(c, jnp.where(exposure == e, 1.0, 0.0))
        early_copy(c).start()

    @pl.loop(early, AHEAD)
    def _(c):
        columns(c + 2)
        resample(c)

    @pl.loop(1, dev_count)
    def _(i):
        weight_copy(i).wait()

    weight_got[0] = weight_src[...]
    weight_sum = jnp.sum(jnp.sum(weight_got[...], axis=0), axis=0, keepdims=True)[:, 0:1]
    average = weight_sum / (exps * dev_count)

    def factor_of(weight):
        return jnp.minimum(weight, clip_ratio * average) / weight

    own_factor = [factor_of(own[e]) for e in range(exps)]
    other = 1 + (dev_count - 2) * (1 - lax.rem(me, 2))
    other_factor = [factor_of(weight_got[other, e : e + 1, 0:1]) for e in range(exps)]
    factor = jnp.zeros((rows, 1), jnp.float32)
    for e in range(exps):
        factor = jnp.where(exposure == e, own_factor[e], factor)

    def stage_copy(b, c, late):
        keep = dev_count >> (b + 1)
        skip = 1 if b == 1 and not late else 0
        source = partial_ref.at[lax.rem(c, ring)] if b == 0 else got_refs[b - 1].at[c]
        return pltpu.make_async_remote_copy(
            src_ref=source.at[pl.ds(keep + skip, keep - skip)],
            dst_ref=got_refs[b].at[c, pl.ds(skip, keep - skip)],
            send_sem=send_sem.at[b, c],
            recv_sem=recv_sem.at[b, c],
            device_id=partner(1 << bit_order(late)[b]),
            device_id_type=MESH,
        )

    def last_copy(c):
        keep = dev_count >> 2
        return pltpu.make_async_remote_copy(
            src_ref=got_refs[0].at[c, pl.ds(keep, 1)],
            dst_ref=got_refs[1].at[c, pl.ds(0, 1)],
            send_sem=last_send.at[c],
            recv_sem=last_recv.at[c],
            device_id=partner(2),
            device_id_type=MESH,
        )

    def start_first(c):
        for late in (False, True):

            @pl.when(is_late(c) if late else jnp.logical_not(is_late(c)))
            def _(late=late):
                stage_copy(1, c, late).start()

    def merge(b, c, late):
        keep = dev_count >> (b + 1)
        stage_copy(b, c, late).wait_recv()
        if b == 0:
            got_refs[0][c] = got_refs[0][c] + partial_ref[lax.rem(c, ring), pl.ds(0, keep)]
        elif b == 1 and not late:
            at = pl.ds(1, keep - 1)
            got_refs[1][c, at] = got_refs[1][c, at] + got_refs[0][c, at]
        elif b == 2 and not late:
            got_refs[2][c, pl.ds(0, 1)] = got_refs[2][c, pl.ds(0, 1)] + got_refs[0][c, pl.ds(0, 1)]
            if keep > 1:
                at = pl.ds(1, keep - 1)
                got_refs[2][c, at] = got_refs[2][c, at] + got_refs[1][c, at]
        elif b < bits - 1:
            got_refs[b][c] = got_refs[b][c] + got_refs[b - 1][c, pl.ds(0, keep)]
        if b == 0:
            start_first(c)
            return
        if b < bits - 1:
            stage_copy(b + 1, c, late).start()
            return
        total = got_refs[b][c, 0] + got_refs[b - 1][c, 0]
        if not late:
            last_copy(c).wait_recv()
            total = total + got_refs[1][c, 0]
        at = pl.ds(pl.multiple_of(c * width, LANES), width)
        numerator = total[:tile_dev]
        denominator = total[tile_dev:]
        positive = denominator > 0
        coadd_ref[:, at] = jnp.where(
            positive, numerator / jnp.where(positive, denominator, 1.0), 0.0
        )
        depth_ref[:, at] = denominator

    def produce(c):
        if ring < chunks:

            @pl.when(c >= ring)
            def _():
                stage_copy(0, c - ring, False).wait_send()

        partial_ref[lax.rem(c, ring)] = partial_of(c, factor)
        stage_copy(0, c, False).start()

    def merge_early(c):
        early_copy(c).wait_recv()

        @pl.loop(0, dev_count // 2)
        def _(j):
            total = None
            for source, scale in ((early_ref, own_factor), (early_got, other_factor)):
                for e in range(exps):
                    term = source[c, e, j] * scale[e]
                    total = term if total is None else total + term
            got_refs[0][c, j] = total

        start_first(c)

    lags, late_lags = stage_lags(LAGS, bits), stage_lags(LATE_LAGS, bits)

    @pl.loop(0, chunks + max(lags[-1], late_lags[-1]))
    def _(step):
        @pl.when((step >= AHEAD) & (step < chunks))
        def _():
            columns(step + 2)
            resample(step)

        @pl.when((step >= early) & (step < chunks))
        def _():
            produce(step)

        @pl.when((step >= lags[0]) & (step < early + lags[0])) if early else unused
        def _():
            merge_early(step - lags[0])

        @pl.when((step >= early + lags[0]) & (step < chunks + lags[0]))
        def _():
            merge(0, step - lags[0], False)

        for b in range(1, bits):
            for late in (False, True):
                c = step - (late_lags if late else lags)[b]
                kind_here = is_late(c) if late else jnp.logical_not(is_late(c))

                @pl.when((c >= 0) & (c < chunks) & kind_here)
                def _(b=b, c=c, late=late):
                    merge(b, c, late)

        for i in range(LAST_PER_STEP):
            c = (step - chunks - LAST_FROM) * LAST_PER_STEP + i

            @pl.when((c >= 0) & (c < chunks) & jnp.logical_not(is_late(c)))
            def _(c=c):
                last_copy(c).start()

    @pl.loop(0, early) if early else unused
    def _(c):
        early_copy(c).wait_send()

    @pl.loop(max(chunks - ring, early), chunks)
    def _(c):
        stage_copy(0, c, False).wait_send()

    @pl.loop(0, chunks)
    def _(c):
        for late in (False, True):

            @pl.when(is_late(c) if late else jnp.logical_not(is_late(c)))
            def _(late=late):
                for b in range(1, bits):
                    stage_copy(b, c, late).wait_send()
                if not late:
                    last_copy(c).wait_send()


def shards(cutouts, variance, offsets, correlation_tiles, slot_valid, tile_slot):
    dev_count = lax.axis_size("exp")
    exps, slots, pixels = cutouts.shape
    rows = exps * slots
    tile_total = tile_slot.shape[0]
    tile_dev = tile_total // dev_count
    bits = dev_count.bit_length() - 1
    chunks = P_SIZE // ROWS
    width = ROWS * P_SIZE
    roomy = dev_count <= ALL_RING
    ring, early = (chunks, EARLY) if roomy else (min(chunks, 4), 0)
    depth = PARTS * (-(-2 * rows // PAD) * PAD)

    def early_shape(blocks):
        return (early, exps, blocks, 2 * tile_dev, width) if early else (ROWS, LANES)

    area = P_SIZE * P_SIZE

    lanes = max(LANES, tile_total)
    small = jnp.concatenate(
        [
            jnp.pad(a, ((0, 0), (0, lanes - a.shape[1])))
            for a in (
                jnp.swapaxes(offsets, 1, 2).reshape(2 * exps, slots),
                correlation_tiles,
                slot_valid,
                tile_slot.reshape(1, tile_total),
            )
        ],
        axis=0,
    )
    whole = pl.BlockSpec(memory_space=pltpu.VMEM)
    far = pl.BlockSpec(memory_space=pltpu.HBM)
    coadd, depth_sum = pl.pallas_call(
        functools.partial(coadd_kernel, dev_count, bits, tile_total, early),
        out_shape=(jax.ShapeDtypeStruct((tile_dev, area), jnp.float32),) * 2,
        in_specs=[far] * 2 + [whole],
        out_specs=(whole,) * 2,
        scratch_shapes=[
            pltpu.VMEM((rows, pixels), cutouts.dtype),
            pltpu.VMEM((rows, pixels), variance.dtype),
            pltpu.VMEM((ROWS, LANES), jnp.float32),
            pltpu.VMEM((dev_count, ROWS, LANES), jnp.float32),
            pltpu.VMEM((2, 2, TAPS, rows, LANES), jnp.float32),
            pltpu.VMEM((rows, CP * P_SIZE), jnp.float32),
            pltpu.VMEM((rows, CP * P_SIZE), jnp.float32),
            pltpu.VMEM((2 * rows, area), jnp.float32),
            pltpu.VMEM(early_shape(dev_count), jnp.float32),
            pltpu.VMEM(early_shape(dev_count // 2), jnp.float32),
            pltpu.VMEM((depth, 2 * tile_total), jnp.float32),
            pltpu.VMEM((2, 2 * tile_total, depth), jnp.bfloat16),
            pltpu.VMEM((depth, width), jnp.bfloat16),
            pltpu.VMEM((ring, dev_count, 2 * tile_dev, width), jnp.float32),
        ]
        + [
            pltpu.VMEM((chunks, dev_count >> (b + 1), 2 * tile_dev, width), jnp.float32)
            for b in range(bits)
        ]
        + [
            pltpu.SemaphoreType.DMA((2, slots)),
            pltpu.SemaphoreType.DMA((dev_count,)),
            pltpu.SemaphoreType.DMA((dev_count,)),
            pltpu.SemaphoreType.DMA((bits, chunks)),
            pltpu.SemaphoreType.DMA((bits, chunks)),
            pltpu.SemaphoreType.DMA((chunks,)),
            pltpu.SemaphoreType.DMA((chunks,)),
        ],
        compiler_params=pltpu.CompilerParams(
            collective_id=0, has_side_effects=True, vmem_limit_bytes=VMEM_LIMIT if roomy else VMEM_MOST
        ),
        name="coadd",
    )(
        jnp.swapaxes(cutouts, 0, 1),
        jnp.swapaxes(variance, 0, 1),
        small,
    )
    shape = (tile_dev, P_SIZE, P_SIZE)
    return (coadd.reshape(shape), depth_sum.reshape(shape))


def solution(mesh):
    in_specs = (
        P(("groups", "exp"), None, None),
        P(("groups", "exp"), None, None),
        P(("groups", "exp"), None, None),
        P(("groups", "exp"), None),
        P(("groups", "exp"), None),
        P("groups"),
    )
    out_specs = (P(("groups", "exp"), None, None), P(("groups", "exp"), None, None))
    return jax.shard_map(shards, mesh=mesh, in_specs=in_specs, out_specs=out_specs, check_vma=False)
```

```python
import functools

import jax
import jax.numpy as jnp
import numpy as np
from jax import lax
from jax.experimental import pallas as pl
from jax.experimental.pallas import tpu as pltpu
from jax.sharding import PartitionSpec as P

P_SIZE = 128
CP = 144
NOFF = 16
TAPS = 6
FIRST = 6
LANES = 128
ROWS = 8
PAD = 16
PARTS = 2
ALL_RING = 16
AHEAD = 3
RAW = 2
RAW_AT = 4
RAW_LAGS = (8, 14)
LATE = (1, 4)
LAGS = (1, 3, 6, 16)
LATE_LAGS = (1, 5, 8, 16)
LAST_FROM = -3
LAST_PER_STEP = 4
VMEM_LIMIT = 55_800_000
VMEM_MOST = 60 * 1024 * 1024
clip_ratio = 1.5
MESH = pl.DeviceIdType.MESH


def tap_table():
    spread = 8.0 + np.arange(NOFF)[:, None] / NOFF - (FIRST + np.arange(TAPS))[None, :]
    table = np.where(np.abs(spread) < 3.0, np.sinc(spread) * np.sinc(spread / 3.0), 0.0)
    return table.astype(np.float32)


TABLE = tap_table()


def pick_taps(offset):
    taps = []
    for t in range(TAPS):
        value = jnp.zeros(offset.shape, jnp.float32)
        for o in range(NOFF):
            value = jnp.where(offset == o, float(TABLE[o, t]), value)
        taps.append(value)
    return taps


def stage_lags(lags, bits):
    middle = [lags[2] + 4 * i for i in range(bits - 3)]
    return list(lags[:2]) + middle + [middle[-1] + lags[3] - lags[2]]


def coadd_kernel(
    dev_count, bits, slot_total, raw, cut_hbm, var_hbm, small_ref,
    coadd_ref, depth_ref, cut_ref, var_ref, weight_src, weight_got, taps_ref,
    cut_mid, var_mid, value_ref, raw_got, table_ref, table_got, pick_other, pick_wide, pick_ref, parts_ref, partial_ref, *rest,
):
    got_refs = rest[:bits]
    load_sem, weight_send, weight_recv, send_sem, recv_sem, last_send, last_recv, raw_sem = rest[bits:]
    slots, exps, _ = cut_hbm.shape
    rows = slots * exps
    tile_dev = slot_total // dev_count
    width = ROWS * P_SIZE
    chunks = P_SIZE // ROWS
    span = ROWS * CP
    ring = partial_ref.shape[0]
    pad = pick_wide.shape[0] // PARTS
    me = lax.axis_index("exp")

    def bit_order(late):
        return [0, *range(2, bits), 1] if late else list(range(bits))

    barrier = pltpu.get_barrier_semaphore()

    @pl.loop(1, dev_count)
    def _(i):
        pl.semaphore_signal(
            barrier, inc=1, device_id={"exp": lax.rem(me + i, dev_count)}, device_id_type=MESH
        )

    def load(kind, s):
        source, to = ((cut_hbm, cut_ref), (var_hbm, var_ref))[kind]
        return pltpu.make_async_copy(
            source.at[s], to.at[pl.ds(s * exps, exps)], load_sem.at[kind, s]
        )

    for kind in (1, 0):
        for s in range(slots):
            load(kind, s).start()

    of_row = lax.broadcasted_iota(jnp.int32, (rows, slots), 0)
    of_slot = lax.broadcasted_iota(jnp.int32, (rows, slots), 1) == of_row // exps

    def by_row(values):
        column = jnp.zeros((rows, slots), jnp.float32)
        for e in range(exps):
            here = of_slot & (of_row % exps == e)
            column = column + jnp.where(here, values[e].astype(jnp.float32), 0.0)
        return jnp.sum(column, axis=1, keepdims=True)

    def small_row(i):
        return small_ref[i : i + 1, :slots]

    offsets = [by_row([small_row(2 * e + axis) for e in range(exps)]) for axis in range(2)]
    tile = by_row([small_row(2 * exps + e) for e in range(exps)])
    valid = by_row([small_row(3 * exps + e) for e in range(exps)])

    for s in range(slots):
        load(1, s).wait()

    def add_up(g, total):
        var = var_ref[:, pl.ds(pl.multiple_of(g * span, LANES), span)].astype(jnp.float32)
        for k in range(span // LANES):
            total = total + var[:, k * LANES : (k + 1) * LANES]
        return total

    sums = lax.fori_loop(0, CP // ROWS, add_up, jnp.zeros((rows, LANES), jnp.float32))

    exposure = lax.broadcasted_iota(jnp.int32, (rows, 1), 0) % exps
    row_total = jnp.sum(sums, axis=1, keepdims=True) * valid
    own = []
    for e in range(exps):
        total = jnp.sum(jnp.where(exposure == e, row_total, 0.0), axis=0, keepdims=True)
        count = jnp.sum(jnp.where(exposure == e, valid, 0.0), axis=0, keepdims=True)
        own.append(1.0 / (total / (count * (CP * CP))))
    weight_row = lax.broadcasted_iota(jnp.int32, weight_src.shape, 0)
    weight_src[...] = functools.reduce(
        lambda a, b: a + b, [jnp.where(weight_row == e, own[e], 0.0) for e in range(exps)]
    )
    pl.semaphore_wait(barrier, dev_count - 1)

    def weight_copy(i):
        return pltpu.make_async_remote_copy(
            src_ref=weight_src,
            dst_ref=weight_got.at[i],
            send_sem=weight_send.at[i],
            recv_sem=weight_recv.at[i],
            device_id={"exp": lax.rem(me + i, dev_count)},
            device_id_type=MESH,
        )

    @pl.loop(1, dev_count)
    def _(i):
        weight_copy(i).start()

    for axis in range(2):
        taps = pick_taps(jnp.broadcast_to(offsets[axis], (rows, LANES)))
        for t in range(TAPS):
            taps_ref[axis, 0, t] = taps[t]
            taps_ref[axis, 1, t] = taps[t] * taps[t]

    lane = lax.broadcasted_iota(jnp.int32, (rows, LANES), 1)

    def shifted(blocks, by):
        turned = [pltpu.roll(block, LANES - by, axis=1) for block in blocks]
        return [
            jnp.where(lane < LANES - by, here, beyond)
            for here, beyond in zip(turned, turned[1:] + turned[-1:])
        ]

    def columns(g):
        at = pl.ds(pl.multiple_of(g * span, LANES), span)
        for kind in range(2):
            data = (cut_ref, var_ref)[kind][:, at].astype(jnp.float32)
            mid = (cut_mid, var_mid)[kind]
            first = [data[:, k * LANES : (k + 1) * LANES] for k in range(span // LANES)]
            second, third = shifted(first, 1), shifted(first, 2)
            tap = [taps_ref[1, kind, t] for t in range(TAPS)]
            low, high = (
                [tap[t] * x + tap[t + 1] * y + tap[t + 2] * z for x, y, z in zip(first, second, third)]
                for t in (0, 3)
            )
            for r in range(ROWS):
                got = None
                for part, start in ((low, FIRST), (high, FIRST + 3)):
                    block, by = divmod(r * CP + start, LANES)
                    near = pltpu.roll(part[block], LANES - by, axis=1)
                    far = pltpu.roll(part[block + 1], LANES - by, axis=1)
                    term = jnp.where(lane < LANES - by, near, far)
                    got = term if got is None else got + term
                mid[:, pl.ds(pl.multiple_of((g * ROWS + r) * LANES, LANES), LANES)] = got

    row = lax.broadcasted_iota(jnp.int32, (rows, 2 * slot_total), 1)
    place = row // (2 * tile_dev)
    kind_of = (row // tile_dev) % 2
    tile_ids = lax.broadcasted_iota(jnp.int32, (rows, slot_total), 1)
    storage = jnp.sum(
        jnp.where(tile == tile_ids.astype(jnp.float32), small_ref[4 * exps : 4 * exps + 1, :slot_total].astype(jnp.float32), 0.0),
        axis=1,
        keepdims=True,
    )
    def build_pick(late, stored, target):
        order = bit_order(late)
        owner = jnp.zeros_like(place)
        for b in range(bits):
            apart = (place // (1 << (bits - 1 - b))) % 2
            mine = lax.rem(lax.div(me, 1 << order[b]), 2)
            owner = owner + ((apart + mine) % 2) * (1 << order[b])
        wanted = (owner * tile_dev + row % tile_dev).astype(jnp.float32)
        for kind in range(2):
            hit = jnp.where((kind_of == kind) & (wanted == stored), 1.0, 0.0)
            for part in range(PARTS):
                base = part * pad + kind * rows
                pick_wide[base : base + rows, :] = hit
        target[late] = pick_wide[...].T.astype(jnp.bfloat16)

    def partner(stride):
        return {"exp": me + (1 - 2 * lax.rem(lax.div(me, stride), 2)) * stride}

    def raw_copy(which, i):
        at = pl.ds(pl.multiple_of(i * width, LANES), width)
        return pltpu.make_async_remote_copy(
            src_ref=(table_ref, value_ref.at[:, at])[which],
            dst_ref=(table_got, raw_got)[which].at[i],
            send_sem=raw_sem.at[2 * which, i],
            recv_sem=raw_sem.at[2 * which + 1, i],
            device_id=partner(2 + 2 * i),
            device_id_type=MESH,
        )

    stored_here = jnp.where(valid > 0, storage, -1.0)
    table_ref[...] = jnp.broadcast_to(stored_here, table_ref.shape)
    if raw:
        for i in range(RAW):
            raw_copy(0, i).start()
    for s in range(slots):
        load(0, s).wait()

    def resample(c):
        for r in range(ROWS):
            value = []
            for kind in range(2):
                mid = (cut_mid, var_mid)[kind]
                got = None
                for t in range(TAPS):
                    from_row = c * ROWS + r + FIRST + t
                    at = pl.ds(pl.multiple_of(from_row * LANES, LANES), LANES)
                    term = taps_ref[0, kind, t] * mid[:, at]
                    got = term if t == 0 else got + term
                value.append(got)
            inverse = 1.0 / value[1]
            at = pl.ds(pl.multiple_of(c * width + r * LANES, LANES), LANES)
            value_ref[:rows, at] = value[0] * inverse
            value_ref[rows:, at] = inverse

    columns(0)
    columns(1)

    if raw:

        @pl.loop(0, raw)
        def _(c):
            columns(c + 2)
            resample(c)
            raw_copy(1, c).start()

    def is_late(c):
        return functools.reduce(lambda a, b: a | b, [c == late for late in LATE])

    def partial_of(read, scale, pick):
        both = jnp.concatenate([scale, scale], axis=0)
        for r in range(ROWS):
            piece_of = read(r) * both
            for part in range(PARTS):
                piece = piece_of.astype(jnp.bfloat16)
                parts_ref[part * pad : part * pad + 2 * rows, r * LANES : (r + 1) * LANES] = piece
                piece_of = piece_of - piece.astype(jnp.float32)
        added = jnp.dot(pick, parts_ref[...], preferred_element_type=jnp.float32)
        return added.reshape(dev_count, 2 * tile_dev, width)

    def own_values(c):
        return lambda r: value_ref[:, pl.ds(pl.multiple_of(c * width + r * LANES, LANES), LANES)]

    pick_wide[...] = jnp.zeros_like(pick_wide)
    parts_ref[...] = jnp.zeros_like(parts_ref)
    for late in range(2):
        build_pick(late, stored_here, pick_ref)

    @pl.loop(raw, AHEAD)
    def _(c):
        columns(c + 2)
        resample(c)

    if raw:
        for i in range(RAW):
            raw_copy(0, i).wait_recv()
            build_pick(i, table_got[i, :, 0:1], pick_other)

    @pl.loop(1, dev_count)
    def _(i):
        weight_copy(i).wait()

    weight_got[0] = weight_src[...]
    weight_sum = jnp.sum(jnp.sum(weight_got[...], axis=0), axis=0, keepdims=True)[:, 0:1]
    average = weight_sum / (exps * dev_count)

    def factor_of(weight):
        return jnp.minimum(weight, clip_ratio * average) / weight

    def spread(weights):
        column = jnp.zeros((rows, 1), jnp.float32)
        for e in range(exps):
            column = jnp.where(exposure == e, factor_of(weights[e]), column)
        return column

    def weights_of(stride):
        i = stride + (dev_count - 2 * stride) * (1 - lax.rem(lax.div(me, stride), 2))
        return [weight_got[i, e : e + 1, 0:1] for e in range(exps)]

    factor = spread(own)

    def stage_copy(b, c, late):
        keep = dev_count >> (b + 1)
        skip = 1 if b == 1 and not late else 0
        source = partial_ref.at[lax.rem(c, ring)] if b == 0 else got_refs[b - 1].at[c]
        return pltpu.make_async_remote_copy(
            src_ref=source.at[pl.ds(keep + skip, keep - skip)],
            dst_ref=got_refs[b].at[c, pl.ds(skip, keep - skip)],
            send_sem=send_sem.at[b, c],
            recv_sem=recv_sem.at[b, c],
            device_id=partner(1 << bit_order(late)[b]),
            device_id_type=MESH,
        )

    def last_copy(c):
        keep = dev_count >> 2
        return pltpu.make_async_remote_copy(
            src_ref=got_refs[0].at[c, pl.ds(keep, 1)],
            dst_ref=got_refs[1].at[c, pl.ds(0, 1)],
            send_sem=last_send.at[c],
            recv_sem=last_recv.at[c],
            device_id=partner(2),
            device_id_type=MESH,
        )

    def start_first(c):
        for late in (False, True):

            @pl.when(is_late(c) if late else jnp.logical_not(is_late(c)))
            def _(late=late):
                stage_copy(1, c, late).start()

    def merge(b, c, late, whole=False):
        keep = dev_count >> (b + 1)
        stage_copy(b, c, late).wait_recv()
        if b == 0:
            got_refs[0][c] = got_refs[0][c] + partial_ref[lax.rem(c, ring), pl.ds(0, keep)]
        elif b == 1 and not late:
            at = pl.ds(1, keep - 1)
            got_refs[1][c, at] = got_refs[1][c, at] + got_refs[0][c, at]
        elif b == 2 and not late and not whole:
            got_refs[2][c, pl.ds(0, 1)] = got_refs[2][c, pl.ds(0, 1)] + got_refs[0][c, pl.ds(0, 1)]
            if keep > 1:
                at = pl.ds(1, keep - 1)
                got_refs[2][c, at] = got_refs[2][c, at] + got_refs[1][c, at]
        elif b < bits - 1:
            got_refs[b][c] = got_refs[b][c] + got_refs[b - 1][c, pl.ds(0, keep)]
        if b == 0:
            start_first(c)
            return
        if b < bits - 1:
            stage_copy(b + 1, c, late).start()
            return
        total = got_refs[b][c, 0] + got_refs[b - 1][c, 0]
        if not late and not whole:
            last_copy(c).wait_recv()
            total = total + got_refs[1][c, 0]
        at = pl.ds(pl.multiple_of(c * width, LANES), width)
        numerator = total[:tile_dev]
        denominator = total[tile_dev:]
        positive = denominator > 0
        coadd_ref[:, at] = jnp.where(
            positive, numerator / jnp.where(positive, denominator, 1.0), 0.0
        )
        depth_ref[:, at] = denominator

    def produce(c):
        if ring < chunks:

            @pl.when(c >= ring)
            def _():
                stage_copy(0, c - ring, False).wait_send()

        pick = pick_ref[is_late(c).astype(jnp.int32)]
        partial_ref[lax.rem(c, ring)] = partial_of(own_values(c), factor, pick)
        stage_copy(0, c, False).start()

    def raw_core(i):
        quarter = dev_count // 4
        return pltpu.make_async_remote_copy(
            src_ref=partial_ref.at[i, pl.ds(dev_count // 2, quarter)],
            dst_ref=got_refs[1].at[i],
            send_sem=send_sem.at[0, i],
            recv_sem=recv_sem.at[0, i],
            device_id=partner(1),
            device_id_type=MESH,
        )

    def raw_produce(i):
        partial_ref[i] = partial_of(own_values(i), factor, pick_ref[i])
        raw_copy(1, i).wait_recv()
        there = spread(weights_of(2 + 2 * i))
        added = partial_of(
            lambda r: raw_got[i, :, r * LANES : (r + 1) * LANES], there, pick_other[i]
        )
        partial_ref[i] = partial_ref[i] + added
        raw_core(i).start()

    def raw_merge(i):
        raw_core(i).wait_recv()
        got_refs[1][i] = got_refs[1][i] + partial_ref[i, pl.ds(0, dev_count // 4)]
        stage_copy(2, i, bool(i)).start()

    lags, late_lags = stage_lags(LAGS, bits), stage_lags(LATE_LAGS, bits)
    first = 1 - raw

    def is_split(c):
        return jnp.logical_not(is_late(c)) & (c >= raw)

    @pl.loop(0, chunks + max(lags[-1], late_lags[-1]))
    def _(step):
        made = step + raw

        @pl.when((made >= AHEAD) & (made < chunks))
        def _():
            columns(made + 2)
            resample(made)

        @pl.when(made < chunks)
        def _():
            produce(made)

        @pl.when((step >= raw + first) & (step < chunks + first))
        def _():
            merge(0, step - first, False)

        if raw:
            for i in range(RAW):

                @pl.when(step == RAW_AT)
                def _(i=i):
                    raw_produce(i)

            for i in range(RAW):

                @pl.when(step == RAW_AT + 1)
                def _(i=i):
                    raw_merge(i)

            for b in range(2, bits):

                @pl.when(step == RAW_LAGS[b - 2])
                def _(b=b):
                    merge(b, 0, False, True)

        for b in range(1, bits):
            for late in (False, True):
                c = step - (late_lags if late else lags)[b]
                here = is_late(c) if late else is_split(c)
                if late and b == 1:
                    here = here & (c >= raw)

                @pl.when((c >= 0) & (c < chunks) & here)
                def _(b=b, c=c, late=late):
                    merge(b, c, late)

        for i in range(LAST_PER_STEP):
            c = (step - chunks - LAST_FROM) * LAST_PER_STEP + i

            @pl.when((c >= 0) & (c < chunks) & is_split(c))
            def _(c=c):
                last_copy(c).start()

    if raw:
        for i in range(RAW):
            raw_core(i).wait_send()
            for which in range(2):
                raw_copy(which, i).wait_send()
            for b in range(2, bits):
                stage_copy(b, i, bool(i)).wait_send()

    @pl.loop(max(chunks - ring, raw), chunks)
    def _(c):
        stage_copy(0, c, False).wait_send()

    @pl.loop(raw, chunks)
    def _(c):
        for late in (False, True):

            @pl.when(is_late(c) if late else jnp.logical_not(is_late(c)))
            def _(late=late):
                for b in range(1, bits):
                    stage_copy(b, c, late).wait_send()
                if not late:
                    last_copy(c).wait_send()


def shards(cutouts, variance, offsets, correlation_tiles, slot_valid, tile_slot):
    dev_count = lax.axis_size("exp")
    exps, slots, pixels = cutouts.shape
    rows = exps * slots
    tile_total = tile_slot.shape[0]
    tile_dev = tile_total // dev_count
    bits = dev_count.bit_length() - 1
    chunks = P_SIZE // ROWS
    width = ROWS * P_SIZE
    roomy = dev_count <= ALL_RING
    ring, raw = (chunks, RAW) if roomy else (min(chunks, 4), 0)
    depth = PARTS * (-(-2 * rows // PAD) * PAD)

    area = P_SIZE * P_SIZE

    lanes = max(LANES, tile_total)
    small = jnp.concatenate(
        [
            jnp.pad(a, ((0, 0), (0, lanes - a.shape[1])))
            for a in (
                jnp.swapaxes(offsets, 1, 2).reshape(2 * exps, slots),
                correlation_tiles,
                slot_valid,
                tile_slot.reshape(1, tile_total),
            )
        ],
        axis=0,
    )
    whole = pl.BlockSpec(memory_space=pltpu.VMEM)
    far = pl.BlockSpec(memory_space=pltpu.HBM)
    coadd, depth_sum = pl.pallas_call(
        functools.partial(coadd_kernel, dev_count, bits, tile_total, raw),
        out_shape=(jax.ShapeDtypeStruct((tile_dev, area), jnp.float32),) * 2,
        in_specs=[far] * 2 + [whole],
        out_specs=(whole,) * 2,
        scratch_shapes=[
            pltpu.VMEM((rows, pixels), cutouts.dtype),
            pltpu.VMEM((rows, pixels), variance.dtype),
            pltpu.VMEM((ROWS, LANES), jnp.float32),
            pltpu.VMEM((dev_count, ROWS, LANES), jnp.float32),
            pltpu.VMEM((2, 2, TAPS, rows, LANES), jnp.float32),
            pltpu.VMEM((rows, CP * P_SIZE), jnp.float32),
            pltpu.VMEM((rows, CP * P_SIZE), jnp.float32),
            pltpu.VMEM((2 * rows, area), jnp.float32),
            pltpu.VMEM((RAW, 2 * rows, width), jnp.float32),
            pltpu.VMEM((rows, LANES), jnp.float32),
            pltpu.VMEM((RAW, rows, LANES), jnp.float32),
            pltpu.VMEM((2, 2 * tile_total, depth), jnp.bfloat16),
            pltpu.VMEM((depth, 2 * tile_total), jnp.float32),
            pltpu.VMEM((2, 2 * tile_total, depth), jnp.bfloat16),
            pltpu.VMEM((depth, width), jnp.bfloat16),
            pltpu.VMEM((ring, dev_count, 2 * tile_dev, width), jnp.float32),
        ]
        + [
            pltpu.VMEM((chunks, dev_count >> (b + 1), 2 * tile_dev, width), jnp.float32)
            for b in range(bits)
        ]
        + [
            pltpu.SemaphoreType.DMA((2, slots)),
            pltpu.SemaphoreType.DMA((dev_count,)),
            pltpu.SemaphoreType.DMA((dev_count,)),
            pltpu.SemaphoreType.DMA((bits, chunks)),
            pltpu.SemaphoreType.DMA((bits, chunks)),
            pltpu.SemaphoreType.DMA((chunks,)),
            pltpu.SemaphoreType.DMA((chunks,)),
            pltpu.SemaphoreType.DMA((4, RAW)),
        ],
        compiler_params=pltpu.CompilerParams(
            collective_id=0, has_side_effects=True, vmem_limit_bytes=VMEM_LIMIT if roomy else VMEM_MOST
        ),
        name="coadd",
    )(
        jnp.swapaxes(cutouts, 0, 1),
        jnp.swapaxes(variance, 0, 1),
        small,
    )
    shape = (tile_dev, P_SIZE, P_SIZE)
    return (coadd.reshape(shape), depth_sum.reshape(shape))


def solution(mesh):
    in_specs = (
        P(("groups", "exp"), None, None),
        P(("groups", "exp"), None, None),
        P(("groups", "exp"), None, None),
        P(("groups", "exp"), None),
        P(("groups", "exp"), None),
        P("groups"),
    )
    out_specs = (P(("groups", "exp"), None, None), P(("groups", "exp"), None, None))
    return jax.shard_map(shards, mesh=mesh, in_specs=in_specs, out_specs=out_specs, check_vma=False)
```

```python
import functools

import jax
import jax.numpy as jnp
import numpy as np
from jax import lax
from jax.experimental import pallas as pl
from jax.experimental.pallas import tpu as pltpu
from jax.sharding import PartitionSpec as P

P_SIZE = 128
CP = 144
NOFF = 16
TAPS = 6
FIRST = 6
LANES = 128
ROWS = 8
PAD = 16
PARTS = 2
ALL_RING = 16
AHEAD = 3
RAW = 2
RAW_AT = 4
RAW_LAGS = (8, 14)
LATE = (1, 4)
LAGS = (1, 3, 6, 16)
LATE_LAGS = (1, 5, 8, 16)
LAST_FROM = -2
LAST_PER_STEP = 3
VMEM_LIMIT = 55_800_000
VMEM_MOST = 60 * 1024 * 1024
clip_ratio = 1.5
MESH = pl.DeviceIdType.MESH


def tap_table():
    spread = 8.0 + np.arange(NOFF)[:, None] / NOFF - (FIRST + np.arange(TAPS))[None, :]
    table = np.where(np.abs(spread) < 3.0, np.sinc(spread) * np.sinc(spread / 3.0), 0.0)
    return table.astype(np.float32)


TABLE = tap_table()


def pick_taps(offset):
    taps = []
    for t in range(TAPS):
        value = jnp.zeros(offset.shape, jnp.float32)
        for o in range(NOFF):
            value = jnp.where(offset == o, float(TABLE[o, t]), value)
        taps.append(value)
    return taps


def stage_lags(lags, bits):
    middle = [lags[2] + 4 * i for i in range(bits - 3)]
    return list(lags[:2]) + middle + [middle[-1] + lags[3] - lags[2]]


def coadd_kernel(
    dev_count, bits, slot_total, raw, cut_hbm, var_hbm, small_ref,
    coadd_ref, depth_ref, cut_ref, var_ref, weight_src, weight_got, taps_ref,
    cut_mid, var_mid, value_ref, raw_got, table_ref, table_got, pick_other, pick_wide, pick_ref, parts_ref, partial_ref, *rest,
):
    got_refs = rest[:bits]
    load_sem, weight_send, weight_recv, send_sem, recv_sem, last_send, last_recv, raw_sem = rest[bits:]
    slots, exps, _ = cut_hbm.shape
    rows = slots * exps
    tile_dev = slot_total // dev_count
    width = ROWS * P_SIZE
    chunks = P_SIZE // ROWS
    span = ROWS * CP
    ring = partial_ref.shape[0]
    pad = pick_wide.shape[0] // PARTS
    me = lax.axis_index("exp")

    def bit_order(late):
        return [0, *range(2, bits), 1] if late else list(range(bits))

    barrier = pltpu.get_barrier_semaphore()

    def load(kind, s):
        source, to = ((cut_hbm, cut_ref), (var_hbm, var_ref))[kind]
        return pltpu.make_async_copy(
            source.at[s], to.at[pl.ds(s * exps, exps)], load_sem.at[kind, s]
        )

    for s in range(slots):
        load(1, s).start()

    @pl.loop(1, dev_count)
    def _(i):
        pl.semaphore_signal(
            barrier, inc=1, device_id={"exp": lax.rem(me + i, dev_count)}, device_id_type=MESH
        )

    for s in range(slots):
        load(0, s).start()

    of_row = lax.broadcasted_iota(jnp.int32, (rows, slots), 0)
    of_slot = lax.broadcasted_iota(jnp.int32, (rows, slots), 1) == of_row // exps

    def by_row(values):
        column = jnp.zeros((rows, slots), jnp.float32)
        for e in range(exps):
            here = of_slot & (of_row % exps == e)
            column = column + jnp.where(here, values[e].astype(jnp.float32), 0.0)
        return jnp.sum(column, axis=1, keepdims=True)

    def small_row(i):
        return small_ref[i : i + 1, :slots]

    offsets = [by_row([small_row(2 * e + axis) for e in range(exps)]) for axis in range(2)]
    tile = by_row([small_row(2 * exps + e) for e in range(exps)])
    valid = by_row([small_row(3 * exps + e) for e in range(exps)])

    for s in range(slots):
        load(1, s).wait()

    def add_up(g, total):
        var = var_ref[:, pl.ds(pl.multiple_of(g * span, LANES), span)].astype(jnp.float32)
        for k in range(span // LANES):
            total = total + var[:, k * LANES : (k + 1) * LANES]
        return total

    sums = lax.fori_loop(0, CP // ROWS, add_up, jnp.zeros((rows, LANES), jnp.float32))

    exposure = lax.broadcasted_iota(jnp.int32, (rows, 1), 0) % exps
    row_total = jnp.sum(sums, axis=1, keepdims=True) * valid
    own = []
    for e in range(exps):
        total = jnp.sum(jnp.where(exposure == e, row_total, 0.0), axis=0, keepdims=True)
        count = jnp.sum(jnp.where(exposure == e, valid, 0.0), axis=0, keepdims=True)
        own.append(1.0 / (total / (count * (CP * CP))))
    weight_row = lax.broadcasted_iota(jnp.int32, weight_src.shape, 0)
    weight_src[...] = functools.reduce(
        lambda a, b: a + b, [jnp.where(weight_row == e, own[e], 0.0) for e in range(exps)]
    )
    pl.semaphore_wait(barrier, dev_count - 1)

    def weight_copy(i):
        return pltpu.make_async_remote_copy(
            src_ref=weight_src,
            dst_ref=weight_got.at[i],
            send_sem=weight_send.at[i],
            recv_sem=weight_recv.at[i],
            device_id={"exp": lax.rem(me + i, dev_count)},
            device_id_type=MESH,
        )

    @pl.loop(1, dev_count)
    def _(i):
        weight_copy(i).start()

    for axis in range(2):
        taps = pick_taps(jnp.broadcast_to(offsets[axis], (rows, LANES)))
        for t in range(TAPS):
            taps_ref[axis, 0, t] = taps[t]
            taps_ref[axis, 1, t] = taps[t] * taps[t]

    lane = lax.broadcasted_iota(jnp.int32, (rows, LANES), 1)

    def shifted(blocks, by):
        turned = [pltpu.roll(block, LANES - by, axis=1) for block in blocks]
        return [
            jnp.where(lane < LANES - by, here, beyond)
            for here, beyond in zip(turned, turned[1:] + turned[-1:])
        ]

    def columns(g):
        at = pl.ds(pl.multiple_of(g * span, LANES), span)
        for kind in range(2):
            data = (cut_ref, var_ref)[kind][:, at].astype(jnp.float32)
            mid = (cut_mid, var_mid)[kind]
            first = [data[:, k * LANES : (k + 1) * LANES] for k in range(span // LANES)]
            second, third = shifted(first, 1), shifted(first, 2)
            tap = [taps_ref[1, kind, t] for t in range(TAPS)]
            low, high = (
                [tap[t] * x + tap[t + 1] * y + tap[t + 2] * z for x, y, z in zip(first, second, third)]
                for t in (0, 3)
            )
            for r in range(ROWS):
                got = None
                for part, start in ((low, FIRST), (high, FIRST + 3)):
                    block, by = divmod(r * CP + start, LANES)
                    near = pltpu.roll(part[block], LANES - by, axis=1)
                    far = pltpu.roll(part[block + 1], LANES - by, axis=1)
                    term = jnp.where(lane < LANES - by, near, far)
                    got = term if got is None else got + term
                mid[:, pl.ds(pl.multiple_of((g * ROWS + r) * LANES, LANES), LANES)] = got

    row = lax.broadcasted_iota(jnp.int32, (rows, 2 * slot_total), 1)
    place = row // (2 * tile_dev)
    kind_of = (row // tile_dev) % 2
    tile_ids = lax.broadcasted_iota(jnp.int32, (rows, slot_total), 1)
    storage = jnp.sum(
        jnp.where(tile == tile_ids.astype(jnp.float32), small_ref[4 * exps : 4 * exps + 1, :slot_total].astype(jnp.float32), 0.0),
        axis=1,
        keepdims=True,
    )
    def build_pick(late, stored, target):
        order = bit_order(late)
        owner = jnp.zeros_like(place)
        for b in range(bits):
            apart = (place // (1 << (bits - 1 - b))) % 2
            mine = lax.rem(lax.div(me, 1 << order[b]), 2)
            owner = owner + ((apart + mine) % 2) * (1 << order[b])
        wanted = (owner * tile_dev + row % tile_dev).astype(jnp.float32)
        for kind in range(2):
            hit = jnp.where((kind_of == kind) & (wanted == stored), 1.0, 0.0)
            for part in range(PARTS):
                base = part * pad + kind * rows
                pick_wide[base : base + rows, :] = hit
        target[late] = pick_wide[...].T.astype(jnp.bfloat16)

    def partner(stride):
        return {"exp": me + (1 - 2 * lax.rem(lax.div(me, stride), 2)) * stride}

    def raw_copy(which, i):
        at = pl.ds(pl.multiple_of(i * width, LANES), width)
        return pltpu.make_async_remote_copy(
            src_ref=(table_ref, value_ref.at[:, at])[which],
            dst_ref=(table_got, raw_got)[which].at[i],
            send_sem=raw_sem.at[2 * which, i],
            recv_sem=raw_sem.at[2 * which + 1, i],
            device_id=partner(2 + 2 * i),
            device_id_type=MESH,
        )

    stored_here = jnp.where(valid > 0, storage, -1.0)
    table_ref[...] = jnp.broadcast_to(stored_here, table_ref.shape)
    if raw:
        for i in range(RAW):
            raw_copy(0, i).start()
    for s in range(slots):
        load(0, s).wait()

    def resample(c):
        for r in range(ROWS):
            value = []
            for kind in range(2):
                mid = (cut_mid, var_mid)[kind]
                got = None
                for t in range(TAPS):
                    from_row = c * ROWS + r + FIRST + t
                    at = pl.ds(pl.multiple_of(from_row * LANES, LANES), LANES)
                    term = taps_ref[0, kind, t] * mid[:, at]
                    got = term if t == 0 else got + term
                value.append(got)
            inverse = 1.0 / value[1]
            at = pl.ds(pl.multiple_of(c * width + r * LANES, LANES), LANES)
            value_ref[:rows, at] = value[0] * inverse
            value_ref[rows:, at] = inverse

    columns(0)
    columns(1)

    if raw:

        @pl.loop(0, raw)
        def _(c):
            columns(c + 2)
            resample(c)
            raw_copy(1, c).start()

    def is_late(c):
        return functools.reduce(lambda a, b: a | b, [c == late for late in LATE])

    def partial_of(read, scale, pick):
        both = jnp.concatenate([scale, scale], axis=0)
        for r in range(ROWS):
            piece_of = read(r) * both
            for part in range(PARTS):
                piece = piece_of.astype(jnp.bfloat16)
                parts_ref[part * pad : part * pad + 2 * rows, r * LANES : (r + 1) * LANES] = piece
                piece_of = piece_of - piece.astype(jnp.float32)
        added = jnp.dot(pick, parts_ref[...], preferred_element_type=jnp.float32)
        return added.reshape(dev_count, 2 * tile_dev, width)

    def own_values(c):
        return lambda r: value_ref[:, pl.ds(pl.multiple_of(c * width + r * LANES, LANES), LANES)]

    pick_wide[...] = jnp.zeros_like(pick_wide)
    parts_ref[...] = jnp.zeros_like(parts_ref)
    for late in range(2):
        build_pick(late, stored_here, pick_ref)

    @pl.loop(raw, AHEAD)
    def _(c):
        columns(c + 2)
        resample(c)

    if raw:
        for i in range(RAW):
            raw_copy(0, i).wait_recv()
            build_pick(i, table_got[i, :, 0:1], pick_other)

    @pl.loop(1, dev_count)
    def _(i):
        weight_copy(i).wait()

    weight_got[0] = weight_src[...]
    weight_sum = jnp.sum(jnp.sum(weight_got[...], axis=0), axis=0, keepdims=True)[:, 0:1]
    average = weight_sum / (exps * dev_count)

    def factor_of(weight):
        return jnp.minimum(weight, clip_ratio * average) / weight

    def spread(weights):
        column = jnp.zeros((rows, 1), jnp.float32)
        for e in range(exps):
            column = jnp.where(exposure == e, factor_of(weights[e]), column)
        return column

    def weights_of(stride):
        i = stride + (dev_count - 2 * stride) * (1 - lax.rem(lax.div(me, stride), 2))
        return [weight_got[i, e : e + 1, 0:1] for e in range(exps)]

    factor = spread(own)

    def stage_copy(b, c, late):
        keep = dev_count >> (b + 1)
        skip = 1 if b == 1 and not late else 0
        source = partial_ref.at[lax.rem(c, ring)] if b == 0 else got_refs[b - 1].at[c]
        return pltpu.make_async_remote_copy(
            src_ref=source.at[pl.ds(keep + skip, keep - skip)],
            dst_ref=got_refs[b].at[c, pl.ds(skip, keep - skip)],
            send_sem=send_sem.at[b, c],
            recv_sem=recv_sem.at[b, c],
            device_id=partner(1 << bit_order(late)[b]),
            device_id_type=MESH,
        )

    def last_copy(c):
        keep = dev_count >> 2
        return pltpu.make_async_remote_copy(
            src_ref=got_refs[0].at[c, pl.ds(keep, 1)],
            dst_ref=got_refs[1].at[c, pl.ds(0, 1)],
            send_sem=last_send.at[c],
            recv_sem=last_recv.at[c],
            device_id=partner(2),
            device_id_type=MESH,
        )

    def start_first(c):
        for late in (False, True):

            @pl.when(is_late(c) if late else jnp.logical_not(is_late(c)))
            def _(late=late):
                stage_copy(1, c, late).start()

    def merge(b, c, late, whole=False):
        keep = dev_count >> (b + 1)
        stage_copy(b, c, late).wait_recv()
        if b == 0:
            got_refs[0][c] = got_refs[0][c] + partial_ref[lax.rem(c, ring), pl.ds(0, keep)]
        elif b == 1 and not late:
            at = pl.ds(1, keep - 1)
            got_refs[1][c, at] = got_refs[1][c, at] + got_refs[0][c, at]
        elif b == 2 and not late and not whole:
            got_refs[2][c, pl.ds(0, 1)] = got_refs[2][c, pl.ds(0, 1)] + got_refs[0][c, pl.ds(0, 1)]
            if keep > 1:
                at = pl.ds(1, keep - 1)
                got_refs[2][c, at] = got_refs[2][c, at] + got_refs[1][c, at]
        elif b < bits - 1:
            got_refs[b][c] = got_refs[b][c] + got_refs[b - 1][c, pl.ds(0, keep)]
        if b == 0:
            start_first(c)
            return
        if b < bits - 1:
            stage_copy(b + 1, c, late).start()
            return
        total = got_refs[b][c, 0] + got_refs[b - 1][c, 0]
        if not late and not whole:
            last_copy(c).wait_recv()
            total = total + got_refs[1][c, 0]
        at = pl.ds(pl.multiple_of(c * width, LANES), width)
        numerator = total[:tile_dev]
        denominator = total[tile_dev:]
        positive = denominator > 0
        coadd_ref[:, at] = jnp.where(
            positive, numerator / jnp.where(positive, denominator, 1.0), 0.0
        )
        depth_ref[:, at] = denominator

    def produce(c):
        if ring < chunks:

            @pl.when(c >= ring)
            def _():
                stage_copy(0, c - ring, False).wait_send()

        pick = pick_ref[is_late(c).astype(jnp.int32)]
        partial_ref[lax.rem(c, ring)] = partial_of(own_values(c), factor, pick)
        stage_copy(0, c, False).start()

    def raw_core(i):
        quarter = dev_count // 4
        return pltpu.make_async_remote_copy(
            src_ref=partial_ref.at[i, pl.ds(dev_count // 2, quarter)],
            dst_ref=got_refs[1].at[i],
            send_sem=send_sem.at[0, i],
            recv_sem=recv_sem.at[0, i],
            device_id=partner(1),
            device_id_type=MESH,
        )

    def raw_produce(i):
        partial_ref[i] = partial_of(own_values(i), factor, pick_ref[i])
        raw_copy(1, i).wait_recv()
        there = spread(weights_of(2 + 2 * i))
        added = partial_of(
            lambda r: raw_got[i, :, r * LANES : (r + 1) * LANES], there, pick_other[i]
        )
        partial_ref[i] = partial_ref[i] + added
        raw_core(i).start()

    def raw_merge(i):
        raw_core(i).wait_recv()
        got_refs[1][i] = got_refs[1][i] + partial_ref[i, pl.ds(0, dev_count // 4)]
        stage_copy(2, i, bool(i)).start()

    lags, late_lags = stage_lags(LAGS, bits), stage_lags(LATE_LAGS, bits)
    first = 1 - raw

    def is_split(c):
        return jnp.logical_not(is_late(c)) & (c >= raw)

    @pl.loop(0, chunks + max(lags[-1], late_lags[-1]))
    def _(step):
        made = step + raw

        @pl.when((made >= AHEAD) & (made < chunks))
        def _():
            columns(made + 2)
            resample(made)

        @pl.when(made < chunks)
        def _():
            produce(made)

        @pl.when((step >= raw + first) & (step < chunks + first))
        def _():
            merge(0, step - first, False)

        if raw:
            for i in range(RAW):

                @pl.when(step == RAW_AT)
                def _(i=i):
                    raw_produce(i)

            for i in range(RAW):

                @pl.when(step == RAW_AT + 1)
                def _(i=i):
                    raw_merge(i)

            for b in range(2, bits):

                @pl.when(step == RAW_LAGS[b - 2])
                def _(b=b):
                    merge(b, 0, False, True)

        for b in range(1, bits):
            for late in (False, True):
                c = step - (late_lags if late else lags)[b]
                here = is_late(c) if late else is_split(c)
                if late and b == 1:
                    here = here & (c >= raw)

                @pl.when((c >= 0) & (c < chunks) & here)
                def _(b=b, c=c, late=late):
                    merge(b, c, late)

        for i in range(LAST_PER_STEP):
            c = (step - chunks - LAST_FROM) * LAST_PER_STEP + i

            @pl.when((c >= 0) & (c < chunks) & is_split(c))
            def _(c=c):
                last_copy(c).start()

    if raw:
        for i in range(RAW):
            raw_core(i).wait_send()
            for which in range(2):
                raw_copy(which, i).wait_send()
            for b in range(2, bits):
                stage_copy(b, i, bool(i)).wait_send()

    @pl.loop(max(chunks - ring, raw), chunks)
    def _(c):
        stage_copy(0, c, False).wait_send()

    @pl.loop(raw, chunks)
    def _(c):
        for late in (False, True):

            @pl.when(is_late(c) if late else jnp.logical_not(is_late(c)))
            def _(late=late):
                for b in range(1, bits):
                    stage_copy(b, c, late).wait_send()
                if not late:
                    last_copy(c).wait_send()


def shards(cutouts, variance, offsets, correlation_tiles, slot_valid, tile_slot):
    dev_count = lax.axis_size("exp")
    exps, slots, pixels = cutouts.shape
    rows = exps * slots
    tile_total = tile_slot.shape[0]
    tile_dev = tile_total // dev_count
    bits = dev_count.bit_length() - 1
    chunks = P_SIZE // ROWS
    width = ROWS * P_SIZE
    roomy = dev_count <= ALL_RING
    ring, raw = (chunks, RAW) if roomy else (min(chunks, 4), 0)
    depth = PARTS * (-(-2 * rows // PAD) * PAD)

    area = P_SIZE * P_SIZE

    lanes = max(LANES, tile_total)
    small = jnp.concatenate(
        [
            jnp.pad(a, ((0, 0), (0, lanes - a.shape[1])))
            for a in (
                jnp.swapaxes(offsets, 1, 2).reshape(2 * exps, slots),
                correlation_tiles,
                slot_valid,
                tile_slot.reshape(1, tile_total),
            )
        ],
        axis=0,
    )
    whole = pl.BlockSpec(memory_space=pltpu.VMEM)
    far = pl.BlockSpec(memory_space=pltpu.HBM)
    coadd, depth_sum = pl.pallas_call(
        functools.partial(coadd_kernel, dev_count, bits, tile_total, raw),
        out_shape=(jax.ShapeDtypeStruct((tile_dev, area), jnp.float32),) * 2,
        in_specs=[far] * 2 + [whole],
        out_specs=(whole,) * 2,
        scratch_shapes=[
            pltpu.VMEM((rows, pixels), cutouts.dtype),
            pltpu.VMEM((rows, pixels), variance.dtype),
            pltpu.VMEM((ROWS, LANES), jnp.float32),
            pltpu.VMEM((dev_count, ROWS, LANES), jnp.float32),
            pltpu.VMEM((2, 2, TAPS, rows, LANES), jnp.float32),
            pltpu.VMEM((rows, CP * P_SIZE), jnp.float32),
            pltpu.VMEM((rows, CP * P_SIZE), jnp.float32),
            pltpu.VMEM((2 * rows, area), jnp.float32),
            pltpu.VMEM((RAW, 2 * rows, width), jnp.float32),
            pltpu.VMEM((rows, LANES), jnp.float32),
            pltpu.VMEM((RAW, rows, LANES), jnp.float32),
            pltpu.VMEM((2, 2 * tile_total, depth), jnp.bfloat16),
            pltpu.VMEM((depth, 2 * tile_total), jnp.float32),
            pltpu.VMEM((2, 2 * tile_total, depth), jnp.bfloat16),
            pltpu.VMEM((depth, width), jnp.bfloat16),
            pltpu.VMEM((ring, dev_count, 2 * tile_dev, width), jnp.float32),
        ]
        + [
            pltpu.VMEM((chunks, dev_count >> (b + 1), 2 * tile_dev, width), jnp.float32)
            for b in range(bits)
        ]
        + [
            pltpu.SemaphoreType.DMA((2, slots)),
            pltpu.SemaphoreType.DMA((dev_count,)),
            pltpu.SemaphoreType.DMA((dev_count,)),
            pltpu.SemaphoreType.DMA((bits, chunks)),
            pltpu.SemaphoreType.DMA((bits, chunks)),
            pltpu.SemaphoreType.DMA((chunks,)),
            pltpu.SemaphoreType.DMA((chunks,)),
            pltpu.SemaphoreType.DMA((4, RAW)),
        ],
        compiler_params=pltpu.CompilerParams(
            collective_id=0, has_side_effects=True, vmem_limit_bytes=VMEM_LIMIT if roomy else VMEM_MOST
        ),
        name="coadd",
    )(
        jnp.swapaxes(cutouts, 0, 1),
        jnp.swapaxes(variance, 0, 1),
        small,
    )
    shape = (tile_dev, P_SIZE, P_SIZE)
    return (coadd.reshape(shape), depth_sum.reshape(shape))


def solution(mesh):
    in_specs = (
        P(("groups", "exp"), None, None),
        P(("groups", "exp"), None, None),
        P(("groups", "exp"), None, None),
        P(("groups", "exp"), None),
        P(("groups", "exp"), None),
        P("groups"),
    )
    out_specs = (P(("groups", "exp"), None, None), P(("groups", "exp"), None, None))
    return jax.shard_map(shards, mesh=mesh, in_specs=in_specs, out_specs=out_specs, check_vma=False)
```
